128 devices in a mesh: seq: 32 (over x, y, z_hi), dp: 4 (over z_lo, core).
Axes of the slice: x: 4, y: 4, z: 4 (z_hi: 2, z_lo: 2; z = z_hi * 2 + z_lo), core: 2. Of those that a mesh axis runs over, the one named last changes fastest.
Arguments:
- queries: bfloat16 [4, 12288, 2048], P('dp', 'seq'), may hold values from -40 to 40
- keys: bfloat16 [4, 12288, 2048], P('dp', 'seq'), may hold values from -40 to 40
- values: bfloat16 [4, 12288, 2048], P('dp', 'seq'), may hold values from -6 to 6
- out_grad: bfloat16 [4, 12288, 2048], P('dp', 'seq'), may hold values from -6 to 6
- proj_weight: bfloat16 [2048, 2048], P('dp'), may hold values from -0.125 to 0.125
- lengths: int32 [4], P('dp'), may hold values from 3072 to 12288
Outputs:
- query_grad: bfloat16 [4, 12288, 2048], P('dp', 'seq')
- key_grad: bfloat16 [4, 12288, 2048], P('dp', 'seq')
- value_grad: bfloat16 [4, 12288, 2048], P('dp', 'seq')
- weight_grad: float32 [2048, 2048], P('dp', 'seq')
The draws below stay inside these ranges and needn't reach their ends.
All inputs are finite; a program needn't handle non-finite values.
Results may differ from the reference program's by a relative error of at most 0.019.
Values may be sent and summed in bfloat16 or wider, within the bound.
A program may use at most 192 MiB of HBM per device.

```python
import jax
import jax.numpy as jnp
from jax import lax

HEADS = 16
HEAD_DIM = 128
DW = 2048
CYCLE = 2
TOK_DEV = 384
FEAT = 2048
TOKENS = 12288
SEQS = 4
N_SEQ = 32


def paired_rows(key):
    base = jax.random.fold_in(key, 7)
    query_draw = jax.random.normal(jax.random.fold_in(base, 1), (SEQS, TOKENS, FEAT), jnp.float32)
    key_draw = jax.random.normal(jax.random.fold_in(base, 2), (SEQS, TOKENS, FEAT), jnp.float32)
    query_draw = jnp.clip(query_draw, -40.0, 40.0)
    key_draw = jnp.clip(key_draw, -40.0, 40.0)
    return (query_draw, key_draw)


def draw_queries(key, part):
    return paired_rows(key)[0].astype(jnp.bfloat16)


def draw_keys(key, part):
    return paired_rows(key)[1].astype(jnp.bfloat16)


def with_ends(values, stream_key, smallest, largest):
    index_at = [jax.random.randint(jax.random.fold_in(stream_key, axis), (), 0, length) for axis, length in enumerate(values.shape)]
    longest = values.shape.index(max(values.shape))
    next_to = index_at[:longest] + [(index_at[longest] + 1) % values.shape[longest]] + index_at[longest + 1:]
    return values.at[tuple(index_at)].set(smallest).at[tuple(next_to)].set(largest)


def strengthened(values, own_key, source, target, shards_of, factor):
    owner, partner = [(jnp.arange(values.shape[dim]) // (values.shape[dim] // shards_of)).reshape([-1 if axis == dim else 1 for axis in range(values.ndim)]) for dim in (source, target)]
    chosen = jax.random.permutation(own_key, shards_of)[partner]
    strong = (owner == chosen) | (owner == (partner + shards_of // 2) % shards_of)
    return jnp.where(strong, factor * values, values)


def level_of(key, extent, pieces, smallest, high):
    gain = 1.0
    for dim, blocks in pieces:
        draws = jax.random.uniform(jax.random.fold_in(jax.random.fold_in(key, 6), dim), (blocks,), jnp.float32, smallest / len(pieces), high / len(pieces))
        gain = gain * jnp.repeat(jnp.exp(draws), extent[dim] // blocks).reshape((-1,) + (1,) * (len(extent) - 1 - dim))
    return gain


def bell_draw(stream_key, dims, spread, most, cuts=(), held_as=jnp.bfloat16):
    drawn = spread * jax.random.normal(stream_key, dims, jnp.float32)
    if cuts:
        drawn = drawn * level_of(stream_key, dims, cuts, -0.22, 0.18)
    return jnp.clip(drawn, -most, most).astype(held_as)


def heavy_noise(rng, shape, deviation, bound, shards, heavy, held_as=jnp.bfloat16):
    drawn = deviation * jax.random.normal(rng, shape, jnp.float32)
    if shards:
        drawn = drawn * level_of(rng, shape, shards, -0.22, 0.18)
    return jnp.clip(strengthened(drawn, jax.random.fold_in(rng, 3), *heavy), -bound, bound).astype(held_as)


def setup_inputs(seed: int = 0) -> dict:
    arg_keys = jax.random.split(jax.random.key(seed), 7)
    return {
        "queries": draw_queries(jax.random.fold_in(arg_keys[6], 71), 0),
        "keys": draw_keys(jax.random.fold_in(arg_keys[6], 71), 0),
        "values": bell_draw(arg_keys[2], (SEQS, TOKENS, FEAT), 1.0, 6.0, ((0, 4), (1, 32))),
        "out_grad": heavy_noise(arg_keys[3], (SEQS, TOKENS, DW), 1.0, 6.0, ((0, 4), (1, 32)), (1, 2, 32, 2.75)),
        "proj_weight": bell_draw(arg_keys[4], (FEAT, DW), FEAT ** -0.5, 0.125, ((0, 4),)),
        "lengths": with_ends(jax.random.randint(arg_keys[5], (SEQS,), TOKENS // 4, TOKENS + 1), jax.random.fold_in(arg_keys[5], 1), TOKENS // 4, TOKENS).astype(jnp.int32),
    }


def reference(queries, keys, values, out_grad, proj_weight, lengths):
    scale = HEAD_DIM ** -0.5
    window = (CYCLE + 1) * TOK_DEV
    leading = CYCLE * TOK_DEV
    weight_total = jnp.zeros((FEAT, DW), jnp.float32)
    query_list = []
    key_list = []
    value_list = []
    for batch in range(SEQS):
        query_seq = queries[batch]
        grad_seq = out_grad[batch]
        front = jnp.zeros((leading, FEAT), jnp.bfloat16)
        key_padded = jnp.concatenate([front, keys[batch]], 0)
        value_padded = jnp.concatenate([front, values[batch]], 0)
        limit = lengths[batch]

        def block_step(carry, index):
            key_accum, value_accum, weight_accum = carry
            first = (index * TOK_DEV).astype(jnp.int32)
            query_block = lax.dynamic_slice_in_dim(query_seq, first, TOK_DEV, 0)
            grad_block = lax.dynamic_slice_in_dim(grad_seq, first, TOK_DEV, 0)
            key_window = lax.dynamic_slice_in_dim(key_padded, first, window, 0)
            value_window = lax.dynamic_slice_in_dim(value_padded, first, window, 0)
            query_pos = first + jnp.arange(TOK_DEV, dtype=jnp.int32)
            key_pos = first - leading + jnp.arange(window, dtype=jnp.int32)
            allowed = (key_pos[None, :] >= 0) & (key_pos[None, :] <= query_pos[:, None])
            query_heads = query_block.reshape(TOK_DEV, HEADS, HEAD_DIM).astype(jnp.float32)
            key_heads = key_window.reshape(window, HEADS, HEAD_DIM).astype(jnp.float32)
            value_heads = value_window.reshape(window, HEADS, HEAD_DIM).astype(jnp.float32)
            scores = jnp.einsum("thd,shd->hts", query_heads, key_heads) * scale
            scores = jnp.where(allowed[None], scores, -1e30)
            maximum = jnp.max(scores, axis=2, keepdims=True)
            lse = maximum + jnp.log(jnp.sum(jnp.exp(scores - maximum), axis=2, keepdims=True))
            probs = jnp.exp(scores - lse)
            probs_b = probs.astype(jnp.bfloat16)
            attn_out = jnp.einsum("hts,shd->thd", probs_b.astype(jnp.float32), value_heads).astype(jnp.bfloat16)
            live = (query_pos < limit).astype(jnp.bfloat16)
            grad_masked = grad_block * live[:, None]
            out_bwd = jnp.dot(grad_masked, proj_weight.T, preferred_element_type=jnp.float32).astype(jnp.bfloat16)
            attn_flat = attn_out.reshape(TOK_DEV, FEAT)
            weight_accum = weight_accum + lax.dot_general(attn_flat, grad_masked, (((0,), (0,)), ((), ())), preferred_element_type=jnp.float32)
            out_heads = out_bwd.reshape(TOK_DEV, HEADS, HEAD_DIM).astype(jnp.float32)
            delta = jnp.sum(out_heads * attn_out.astype(jnp.float32), axis=2)
            prob_grad = jnp.einsum("thd,shd->hts", out_heads, value_heads)
            score_grad = (probs * (prob_grad - delta.T[:, :, None]) * scale).astype(jnp.bfloat16)
            score_f = score_grad.astype(jnp.float32)
            query_grad = jnp.einsum("hts,shd->thd", score_f, key_heads).astype(jnp.bfloat16)
            key_term = jnp.einsum("hts,thd->shd", score_f, query_heads).astype(jnp.bfloat16)
            value_term = jnp.einsum("hts,thd->shd", probs_b.astype(jnp.float32), out_heads).astype(jnp.bfloat16)
            key_old = lax.dynamic_slice_in_dim(key_accum, first, window, 0)
            value_old = lax.dynamic_slice_in_dim(value_accum, first, window, 0)
            key_accum = lax.dynamic_update_slice_in_dim(key_accum, key_old + key_term.reshape(window, FEAT).astype(jnp.float32), first, 0)
            value_accum = lax.dynamic_update_slice_in_dim(value_accum, value_old + value_term.reshape(window, FEAT).astype(jnp.float32), first, 0)
            return (key_accum, value_accum, weight_accum), query_grad.reshape(TOK_DEV, FEAT)

        start_carry = (jnp.zeros((TOKENS + leading, FEAT), jnp.float32), jnp.zeros((TOKENS + leading, FEAT), jnp.float32), weight_total)
        final_carry, query_blocks = lax.scan(block_step, start_carry, jnp.arange(N_SEQ, dtype=jnp.int32))
        key_accum, value_accum, weight_total = final_carry
        query_list.append(query_blocks.reshape(TOKENS, FEAT))
        key_list.append(key_accum[leading:].astype(jnp.bfloat16))
        value_list.append(value_accum[leading:].astype(jnp.bfloat16))
    return (jnp.stack(query_list), jnp.stack(key_list), jnp.stack(value_list), weight_total)
```

```python
import functools

import jax
import jax.numpy as jnp
from jax import lax
from jax.experimental import pallas as pl
from jax.experimental.pallas import tpu as pltpu
from jax.sharding import PartitionSpec as P

HEAD_DIM = 128
LOG2E = 1.4426950408889634
MESH = pl.DeviceIdType.MESH

AB = (((1,), (0,)), ((), ()))
ABT = (((1,), (1,)), ((), ()))


def mm(left, right, dims):
    return lax.dot_general(left, right, dims, preferred_element_type=jnp.float32)


def attention_kernel(
    q_ref,
    k_ref,
    v_ref,
    g_ref,
    w_ref,
    dq_ref,
    dk_ref,
    dv_ref,
    wg_ref,
    q_buf,
    k_buf,
    v_buf,
    g_buf,
    w_buf,
    do_buf,
    at_buf,
    dq_buf,
    kh_buf,
    vh_buf,
    kr_buf,
    vr_buf,
    ko_buf,
    vo_buf,
    kf_buf,
    vf_buf,
    zs_sem,
    kz_sem,
    vz_sem,
    qz_sem,
    g_sem,
    gx_sem,
    w_sem,
    wl_sem,
    ys_sem,
    ky_sem,
    vy_sem,
    rs_sem,
    kr_sem,
    vr_sem,
    os_sem,
    o_sem,
):
    seq = lax.axis_index("seq")
    dp = lax.axis_index("dp")
    columns = lax.axis_size("seq") // 2
    zh = lax.rem(seq, 2)
    col = lax.div(seq, 2)
    zl = lax.div(dp, 2)
    core = lax.rem(dp, 2)
    tokens = q_ref.shape[1]
    half = q_ref.shape[2] // 2
    heads = half // HEAD_DIM
    quarter = w_ref.shape[0]
    scale = HEAD_DIM ** (-0.5)

    def device(col_, zh_, zl_, core_):
        return (2 * col_ + zh_, 2 * zl_ + core_)

    targets = [device(col, core, 1 - zl, t) for t in range(2)]
    homes = [device(col, b, 1 - zl, zh) for b in range(2)]
    following = device(lax.rem(col + 1, columns), zh, zl, core)
    previous = device(lax.rem(col + columns - 1, columns), zh, zl, core)
    partner = device(col, zh, zl, 1 - core)

    barrier = pltpu.get_barrier_semaphore()
    greeted = [following, previous]
    for i in range(1, 8):
        greeted.append(
            device(
                col,
                1 - zh if i & 4 else zh,
                1 - zl if i & 2 else zl,
                1 - core if i & 1 else core,
            )
        )
    for other in greeted:
        pl.semaphore_signal(barrier, inc=1, device_id=other, device_id_type=MESH)
    pl.semaphore_wait(barrier, len(greeted))

    def remote(src, dst, send_sem, recv_sem, to):
        return pltpu.make_async_remote_copy(
            src_ref=src,
            dst_ref=dst,
            send_sem=send_sem,
            recv_sem=recv_sem,
            device_id=to,
            device_id_type=MESH,
        )

    def lanes(h):
        return pl.ds(pl.multiple_of(h * HEAD_DIM, HEAD_DIM), HEAD_DIM)

    my_rows = pl.ds(pl.multiple_of(zh * tokens, tokens), tokens)
    own_rows = pl.ds(2 * tokens, 2 * tokens)
    halo_rows = pl.ds(0, 2 * tokens)
    my_half = pl.ds(pl.multiple_of(core * half, half), half)

    def send_home(ref, buf, base, h, recv_sem, slot):
        rows = pl.ds(pl.multiple_of(base + zh * tokens, tokens), tokens)
        for t in range(2):
            src = pl.ds(pl.multiple_of(t * half + h * HEAD_DIM, HEAD_DIM), HEAD_DIM)
            remote(
                ref.at[0, :, src],
                buf.at[rows, lanes(h)],
                zs_sem.at[slot],
                recv_sem.at[h],
                targets[t],
            ).start()

    send_home(k_ref, k_buf, 2 * tokens, 0, kz_sem, 0)
    send_home(v_ref, v_buf, 2 * tokens, 0, vz_sem, 1)
    for t in range(2):
        cols = pl.ds(t * half, half)
        remote(
            g_ref.at[:, cols],
            g_buf.at[my_rows, cols],
            zs_sem.at[3],
            g_sem,
            targets[t],
        ).start()
    w_rows = pl.ds(pl.multiple_of(core * quarter, quarter), quarter)
    w_local = pltpu.make_async_copy(w_ref, w_buf.at[w_rows], wl_sem)

    def w_send(to):
        return remote(w_ref, w_buf.at[w_rows], zs_sem.at[4], w_sem, to)

    w_far = [device(col, b, 1 - zl, zl) for b in range(2)]

    @pl.when(core == zl)
    def _():
        w_local.start()

    @pl.when(core != zl)
    def _():
        w_send(partner).start()

    @pl.when(zh == core)
    def _():
        for to in w_far:
            w_send(to).start()

    send_home(q_ref, q_buf, 0, 0, qz_sem, 2)

    @pl.loop(1, heads)
    def _(h):
        send_home(k_ref, k_buf, 2 * tokens, h, kz_sem, 0)
        send_home(v_ref, v_buf, 2 * tokens, h, vz_sem, 1)
        send_home(q_ref, q_buf, 0, h, qz_sem, 2)

    def forward(h):
        for buf, got, sem, slot in (
            (k_buf, kz_sem, ky_sem, 0),
            (v_buf, vz_sem, vy_sem, 1),
        ):
            own = buf.at[own_rows, lanes(h)]
            remote(own, own, zs_sem.at[0], got.at[h], partner).wait_recv()
            remote(own, buf.at[halo_rows, lanes(h)], ys_sem.at[slot], sem.at[h], following).start()

    forward(0)

    g_half = g_buf.at[:, my_half]
    remote(g_half, g_half, zs_sem.at[3], g_sem, partner).wait_recv()
    g_swap = remote(g_half, g_half, zs_sem.at[5], gx_sem, partner)
    g_swap.start()

    @pl.when(core == zl)
    def _():
        w_local.wait()
        w_send(partner).wait_recv()

    @pl.when(core != zl)
    def _():
        remote(w_buf, w_buf, zs_sem.at[4], w_sem, partner).wait_recv()

    g_swap.wait_recv()

    @pl.loop(0, 2 * tokens // 256)
    def _(n):
        rows = pl.ds(pl.multiple_of(n * 256, 256), 256)
        do_buf[:, rows] = mm(w_buf[...], g_buf[rows, :], ABT).astype(jnp.bfloat16)

    first = jnp.where(col == 0, -1e30, 0.0).astype(jnp.float32)
    key_pos = lax.broadcasted_iota(jnp.int32, (tokens, tokens), 0)
    query_pos = lax.broadcasted_iota(jnp.int32, (tokens, tokens), 1)

    def head(h):
        at = lanes(h)
        feats = pl.ds(pl.multiple_of(h * HEAD_DIM, HEAD_DIM), HEAD_DIM)
        value_t = v_buf[:, at].T
        key_t = k_buf[:, at].T
        dk = [None] * 4
        dv = [None] * 4

        def add(total, block, term):
            total[block] = term if total[block] is None else total[block] + term

        for b in range(2):
            rows = slice(b * tokens, (b + 1) * tokens)
            q = q_buf[rows, at]
            do = do_buf[feats, rows]
            blocks = [b, b + 1, b + 2]
            tile = [slice(n * tokens, (n + 1) * tokens) for n in blocks]
            scores = []
            for j in range(3):
                s = mm(k_buf[tile[j], at], q, ABT)
                if blocks[j] < 2:
                    s = s + first
                if j == 2:
                    s = jnp.where(key_pos <= query_pos, s, -1e30)
                scores.append(s)
            top = scores[0].max(axis=0, keepdims=True)
            for s in scores[1:]:
                top = jnp.maximum(top, s.max(axis=0, keepdims=True))
            probs = [jnp.exp2((s - top) * (scale * LOG2E)) for s in scores]
            total = probs[0].sum(axis=0, keepdims=True)
            for p in probs[1:]:
                total = total + p.sum(axis=0, keepdims=True)
            inverse = 1.0 / total
            probs = [p * inverse for p in probs]
            attn = None
            for j in range(3):
                probs_b = probs[j].astype(jnp.bfloat16)
                term = mm(value_t[:, tile[j]], probs_b, AB)
                attn = term if attn is None else attn + term
                add(dv, blocks[j], mm(probs_b, do, ABT))
            attn = attn.astype(jnp.bfloat16)
            at_buf[feats, rows] = attn
            delta = jnp.sum(
                do.astype(jnp.float32) * attn.astype(jnp.float32), axis=0, keepdims=True
            )
            dq = None
            for j in range(3):
                grad = mm(v_buf[tile[j], at], do, AB)
                sg = (probs[j] * (grad - delta)).astype(jnp.bfloat16)
                term = mm(key_t[:, tile[j]], sg, AB)
                dq = term if dq is None else dq + term
                add(dk, blocks[j], mm(sg, q, AB))
            dq_buf[rows, at] = (dq * scale).T.astype(jnp.bfloat16)
        for n in range(2):
            rows = slice(n * tokens, (n + 1) * tokens)
            kh_buf[rows, at] = (dk[n] * scale).astype(jnp.bfloat16)
            vh_buf[rows, at] = dv[n].astype(jnp.bfloat16)
            ko_buf[rows, at] = dk[n + 2] * scale
            vo_buf[rows, at] = dv[n + 2]

    def send_out(buf, out, slot, h):
        cols = pl.ds(pl.multiple_of(core * half + h * HEAD_DIM, HEAD_DIM), HEAD_DIM)
        for b in range(2):
            remote(
                buf.at[pl.ds(b * tokens, tokens), lanes(h)],
                out.at[0, :, cols],
                os_sem.at[slot],
                o_sem.at[slot],
                homes[b],
            ).start()

    def finish(h):
        at = lanes(h)
        for got, own, done, out, sem, slot in (
            (kr_buf, ko_buf, kf_buf, dk_ref, kr_sem, 1),
            (vr_buf, vo_buf, vf_buf, dv_ref, vr_sem, 2),
        ):
            piece = got.at[:, at]
            remote(piece, piece, rs_sem.at[0], sem.at[h], partner).wait_recv()
            done[:, at] = (own[:, at] + got[:, at].astype(jnp.float32)).astype(jnp.bfloat16)
            send_out(done, out, slot, h)

    @pl.loop(0, heads)
    def _(h):
        @pl.when(h + 1 < heads)
        def _():
            forward(h + 1)

        at = lanes(h)
        piece = q_buf.at[:, at]
        remote(piece, piece, zs_sem.at[2], qz_sem.at[h], partner).wait_recv()
        for buf, sem in ((k_buf, ky_sem), (v_buf, vy_sem)):
            piece = buf.at[halo_rows, at]
            remote(piece, piece, ys_sem.at[0], sem.at[h], partner).wait_recv()
        head(h)
        for src, dst, sem, slot in ((kh_buf, kr_buf, kr_sem, 0), (vh_buf, vr_buf, vr_sem, 1)):
            remote(
                src.at[:, at], dst.at[:, at], rs_sem.at[slot], sem.at[h], previous
            ).start()
        send_out(dq_buf, dq_ref, 0, h)

        @pl.when(h >= 2)
        def _():
            finish(h - 2)

    @pl.loop(0, wg_ref.shape[1] // 256)
    def _(n):
        cols = pl.ds(pl.multiple_of(n * 256, 256), 256)
        wg_ref[:, cols] = mm(at_buf[...], g_buf[:, cols], AB).astype(jnp.bfloat16)

    finish(heads - 2)
    finish(heads - 1)

    for ref, slot in ((k_ref, 0), (v_ref, 1), (q_ref, 2)):
        remote(ref, ref, zs_sem.at[slot], o_sem.at[0], partner).wait_send()
    remote(g_ref, g_ref, zs_sem.at[3], o_sem.at[0], partner).wait_send()

    @pl.when(core != zl)
    def _():
        w_send(partner).wait_send()

    @pl.when(zh == core)
    def _():
        for to in w_far:
            w_send(to).wait_send()

    g_swap.wait_send()
    for buf, slot in ((kr_buf, 0), (vr_buf, 1)):
        remote(buf, buf, ys_sem.at[slot], o_sem.at[0], partner).wait_send()
        remote(buf, buf, rs_sem.at[slot], o_sem.at[0], partner).wait_send()
    for buf, out, slot in ((dq_buf, dq_ref, 0), (kf_buf, dk_ref, 1), (vf_buf, dv_ref, 2)):
        remote(buf, buf, os_sem.at[slot], o_sem.at[0], partner).wait_send()
        remote(out, out, os_sem.at[slot], o_sem.at[slot], partner).wait_recv()


def attention(queries, keys, values, grad_masked, proj_weight):
    tokens, width = queries.shape[1:]
    half = width // 2
    heads = half // HEAD_DIM
    grad_width = grad_masked.shape[1]
    any_space = pl.BlockSpec(memory_space=pl.ANY)
    dma = pltpu.SemaphoreType.DMA
    bf16 = jnp.bfloat16

    def vmem(rows, cols, dtype=bf16):
        return pltpu.VMEM((rows, cols), dtype)

    pair = vmem(2 * tokens, half)
    outs = jax.ShapeDtypeStruct(queries.shape, bf16)
    return pl.pallas_call(
        attention_kernel,
        out_shape=(outs, outs, outs, jax.ShapeDtypeStruct((half, grad_width), bf16)),
        in_specs=[any_space] * 5,
        out_specs=(any_space, any_space, any_space, pl.BlockSpec(memory_space=pltpu.VMEM)),
        scratch_shapes=[
            pair,
            vmem(4 * tokens, half),
            vmem(4 * tokens, half),
            vmem(2 * tokens, grad_width),
            vmem(half, grad_width),
            vmem(half, 2 * tokens),
            vmem(half, 2 * tokens),
            pair,
            pair,
            pair,
            pair,
            pair,
            vmem(2 * tokens, half, jnp.float32),
            vmem(2 * tokens, half, jnp.float32),
            pair,
            pair,
            dma((6,)),
            dma((heads,)),
            dma((heads,)),
            dma((heads,)),
            dma,
            dma,
            dma,
            dma,
            dma((2,)),
            dma((heads,)),
            dma((heads,)),
            dma((2,)),
            dma((heads,)),
            dma((heads,)),
            dma((3,)),
            dma((3,)),
        ],
        compiler_params=pltpu.CompilerParams(
            collective_id=0, has_side_effects=True, vmem_limit_bytes=66_000_000
        ),
        name="attention",
    )(queries, keys, values, grad_masked, proj_weight)


def reduce_weight(partial):
    blocks = lax.axis_size("seq")
    half, width = partial.shape
    pieces = jnp.moveaxis(partial.reshape(half, blocks, width // blocks), 1, 0)
    arrived = lax.all_to_all(pieces, "seq", split_axis=0, concat_axis=0, tiled=True)
    summed = arrived.astype(jnp.float32).sum(axis=0)
    core = lax.rem(lax.axis_index("dp"), 2)
    rows = summed.reshape(2, half // 2, width // blocks)
    none = jnp.zeros_like(rows)
    padded = jnp.concatenate(
        [jnp.where(core == 0, rows, none), jnp.where(core == 1, rows, none)], axis=0
    )
    parts = lax.all_to_all(padded, "dp", split_axis=0, concat_axis=0, tiled=True)
    return parts.sum(axis=0)


def per_device(queries, keys, values, out_grad, proj_weight, lengths):
    tokens = queries.shape[1]
    position = lax.axis_index("seq")
    query_pos = position * tokens + jnp.arange(tokens, dtype=jnp.int32)
    live = (query_pos < lengths[0]).astype(jnp.bfloat16)
    grad_masked = out_grad[0] * live[:, None]
    dq, dk, dv, partial = attention(queries, keys, values, grad_masked, proj_weight)
    return dq, dk, dv, reduce_weight(partial)


def solution(mesh):
    placed = (
        P("dp", "seq", None),
        P("dp", "seq", None),
        P("dp", "seq", None),
        P("dp", "seq", None),
        P("dp", None),
        P("dp"),
    )
    return jax.shard_map(
        per_device,
        mesh=mesh,
        in_specs=placed,
        out_specs=(
            P("dp", "seq", None),
            P("dp", "seq", None),
            P("dp", "seq", None),
            P("dp", "seq"),
        ),
        check_vma=False,
    )
```

```python
import jax
import jax.numpy as jnp
from jax import lax
from jax.experimental import pallas as pl
from jax.experimental.pallas import tpu as pltpu
from jax.sharding import PartitionSpec as P

HEAD_DIM = 128
LOG2E = 1.4426950408889634
MESH = pl.DeviceIdType.MESH

AB = (((1,), (0,)), ((), ()))
ABT = (((1,), (1,)), ((), ()))


def mm(left, right, dims):
    return lax.dot_general(left, right, dims, preferred_element_type=jnp.float32)


def attention_kernel(
    q_ref,
    k_ref,
    v_ref,
    g_ref,
    w_ref,
    len_ref,
    dq_ref,
    dk_ref,
    dv_ref,
    wg_ref,
    q_buf,
    k_buf,
    v_buf,
    g_buf,
    w_buf,
    do_buf,
    at_buf,
    dq_buf,
    kh_buf,
    vh_buf,
    kr_buf,
    vr_buf,
    ko_buf,
    vo_buf,
    kf_buf,
    vf_buf,
    gm_buf,
    p_buf,
    x1_buf,
    x2_buf,
    y1_buf,
    y2_buf,
    zr_buf,
    gl_sem,
    px_sem,
    x1_sem,
    x2_sem,
    y1_sem,
    y2_sem,
    zr_sem,
    zs_sem,
    kz_sem,
    vz_sem,
    qz_sem,
    g_sem,
    gx_sem,
    w_sem,
    wl_sem,
    ys_sem,
    ky_sem,
    vy_sem,
    rs_sem,
    kr_sem,
    vr_sem,
    os_sem,
    o_sem,
):
    seq = lax.axis_index("seq")
    dp = lax.axis_index("dp")
    columns = lax.axis_size("seq") // 2
    zh = lax.rem(seq, 2)
    col = lax.div(seq, 2)
    zl = lax.div(dp, 2)
    core = lax.rem(dp, 2)
    tokens = q_ref.shape[1]
    half = q_ref.shape[2] // 2
    heads = half // HEAD_DIM
    quarter = w_ref.shape[0]
    scale = HEAD_DIM ** (-0.5)

    def device(col_, zh_, zl_, core_):
        return (2 * col_ + zh_, 2 * zl_ + core_)

    targets = [device(col, core, 1 - zl, t) for t in range(2)]
    homes = [device(col, b, 1 - zl, zh) for b in range(2)]
    following = device(lax.rem(col + 1, columns), zh, zl, core)
    previous = device(lax.rem(col + columns - 1, columns), zh, zl, core)
    partner = device(col, zh, zl, 1 - core)

    g_local = pltpu.make_async_copy(g_ref.at[0], gm_buf, gl_sem)
    g_local.start()

    x_at = lax.div(col, 4)
    y_at = lax.rem(col, 4)

    def pair_of(at, step):
        near = at + 1 - 2 * lax.rem(at, 2)
        turned = lax.rem(core + step, 2)
        return jnp.where(turned == 0, near, 3 - at)

    x_pair = [pair_of(x_at, step) for step in range(2)]
    y_pair = [pair_of(y_at, step) for step in range(2)]
    x_far = lax.rem(x_at + 2, 4)
    y_far = lax.rem(y_at + 2, 4)
    x_dev = [device(4 * n + y_at, zh, zl, core) for n in x_pair]
    y_dev = [device(4 * x_at + n, zh, zl, core) for n in y_pair]

    barrier = pltpu.get_barrier_semaphore()
    greeted = [following, previous, *x_dev, *y_dev]
    for i in range(1, 8):
        greeted.append(
            device(
                col,
                1 - zh if i & 4 else zh,
                1 - zl if i & 2 else zl,
                1 - core if i & 1 else core,
            )
        )
    for other in greeted:
        pl.semaphore_signal(barrier, inc=1, device_id=other, device_id_type=MESH)
    pl.semaphore_wait(barrier, len(greeted))

    def remote(src, dst, send_sem, recv_sem, to):
        return pltpu.make_async_remote_copy(
            src_ref=src,
            dst_ref=dst,
            send_sem=send_sem,
            recv_sem=recv_sem,
            device_id=to,
            device_id_type=MESH,
        )

    def lanes(h):
        return pl.ds(pl.multiple_of(h * HEAD_DIM, HEAD_DIM), HEAD_DIM)

    my_rows = pl.ds(pl.multiple_of(zh * tokens, tokens), tokens)
    own_rows = pl.ds(2 * tokens, 2 * tokens)
    halo_rows = pl.ds(0, 2 * tokens)
    my_half = pl.ds(pl.multiple_of(core * half, half), half)

    def send_home(ref, buf, base, h, recv_sem, slot):
        rows = pl.ds(pl.multiple_of(base + zh * tokens, tokens), tokens)
        for t in range(2):
            src = pl.ds(pl.multiple_of(t * half + h * HEAD_DIM, HEAD_DIM), HEAD_DIM)
            remote(
                ref.at[0, :, src],
                buf.at[rows, lanes(h)],
                zs_sem.at[slot],
                recv_sem.at[h],
                targets[t],
            ).start()

    send_home(k_ref, k_buf, 2 * tokens, 0, kz_sem, 0)
    send_home(v_ref, v_buf, 2 * tokens, 0, vz_sem, 1)
    g_local.wait()
    limit = len_ref[0] - seq * tokens
    live = lax.broadcasted_iota(jnp.int32, gm_buf.shape, 0) < limit
    gm_buf[...] = jnp.where(live, gm_buf[...], jnp.zeros_like(gm_buf))
    for t in range(2):
        cols = pl.ds(t * half, half)
        remote(
            gm_buf.at[:, cols],
            g_buf.at[my_rows, cols],
            zs_sem.at[3],
            g_sem,
            targets[t],
        ).start()
    w_rows = pl.ds(pl.multiple_of(core * quarter, quarter), quarter)
    w_local = pltpu.make_async_copy(w_ref, w_buf.at[w_rows], wl_sem)

    def w_send(to):
        return remote(w_ref, w_buf.at[w_rows], zs_sem.at[4], w_sem, to)

    w_far = [device(col, b, 1 - zl, zl) for b in range(2)]

    @pl.when(core == zl)
    def _():
        w_local.start()

    @pl.when(core != zl)
    def _():
        w_send(partner).start()

    @pl.when(zh == core)
    def _():
        for to in w_far:
            w_send(to).start()

    send_home(q_ref, q_buf, 0, 0, qz_sem, 2)

    @pl.loop(1, heads)
    def _(h):
        send_home(k_ref, k_buf, 2 * tokens, h, kz_sem, 0)
        send_home(v_ref, v_buf, 2 * tokens, h, vz_sem, 1)
        send_home(q_ref, q_buf, 0, h, qz_sem, 2)

    def forward(h):
        for buf, got, sem, slot in (
            (k_buf, kz_sem, ky_sem, 0),
            (v_buf, vz_sem, vy_sem, 1),
        ):
            own = buf.at[own_rows, lanes(h)]
            remote(own, own, zs_sem.at[0], got.at[h], partner).wait_recv()
            remote(own, buf.at[halo_rows, lanes(h)], ys_sem.at[slot], sem.at[h], following).start()

    forward(0)

    g_half = g_buf.at[:, my_half]
    remote(g_half, g_half, zs_sem.at[3], g_sem, partner).wait_recv()
    g_swap = remote(g_half, g_half, zs_sem.at[5], gx_sem, partner)
    g_swap.start()

    @pl.when(core == zl)
    def _():
        w_local.wait()
        w_send(partner).wait_recv()

    @pl.when(core != zl)
    def _():
        remote(w_buf, w_buf, zs_sem.at[4], w_sem, partner).wait_recv()

    g_swap.wait_recv()

    @pl.loop(0, 2 * tokens // 256)
    def _(n):
        rows = pl.ds(pl.multiple_of(n * 256, 256), 256)
        do_buf[:, rows] = mm(w_buf[...], g_buf[rows, :], ABT).astype(jnp.bfloat16)

    first = jnp.where(col == 0, -1e30, 0.0).astype(jnp.float32)
    key_pos = lax.broadcasted_iota(jnp.int32, (tokens, tokens), 0)
    query_pos = lax.broadcasted_iota(jnp.int32, (tokens, tokens), 1)

    def head(h):
        at = lanes(h)
        feats = pl.ds(pl.multiple_of(h * HEAD_DIM, HEAD_DIM), HEAD_DIM)
        value_t = v_buf[:, at].T
        key_t = k_buf[:, at].T
        dk = [None] * 4
        dv = [None] * 4

        def add(total, block, term):
            total[block] = term if total[block] is None else total[block] + term

        for b in range(2):
            rows = slice(b * tokens, (b + 1) * tokens)
            q = q_buf[rows, at]
            do = do_buf[feats, rows]
            blocks = [b, b + 1, b + 2]
            tile = [slice(n * tokens, (n + 1) * tokens) for n in blocks]
            scores = []
            for j in range(3):
                s = mm(k_buf[tile[j], at], q, ABT)
                if blocks[j] < 2:
                    s = s + first
                if j == 2:
                    s = jnp.where(key_pos <= query_pos, s, -1e30)
                scores.append(s)
            top = scores[0].max(axis=0, keepdims=True)
            for s in scores[1:]:
                top = jnp.maximum(top, s.max(axis=0, keepdims=True))
            probs = [jnp.exp2((s - top) * (scale * LOG2E)) for s in scores]
            total = probs[0].sum(axis=0, keepdims=True)
            for p in probs[1:]:
                total = total + p.sum(axis=0, keepdims=True)
            inverse = 1.0 / total
            probs = [p * inverse for p in probs]
            attn = None
            for j in range(3):
                probs_b = probs[j].astype(jnp.bfloat16)
                term = mm(value_t[:, tile[j]], probs_b, AB)
                attn = term if attn is None else attn + term
                add(dv, blocks[j], mm(probs_b, do, ABT))
            attn = attn.astype(jnp.bfloat16)
            at_buf[feats, rows] = attn
            delta = jnp.sum(
                do.astype(jnp.float32) * attn.astype(jnp.float32), axis=0, keepdims=True
            )
            dq = None
            for j in range(3):
                grad = mm(v_buf[tile[j], at], do, AB)
                sg = (probs[j] * (grad - delta)).astype(jnp.bfloat16)
                term = mm(key_t[:, tile[j]], sg, AB)
                dq = term if dq is None else dq + term
                add(dk, blocks[j], mm(sg, q, AB))
            dq_buf[rows, at] = (dq * scale).T.astype(jnp.bfloat16)
        for n in range(2):
            rows = slice(n * tokens, (n + 1) * tokens)
            kh_buf[rows, at] = (dk[n] * scale).astype(jnp.bfloat16)
            vh_buf[rows, at] = dv[n].astype(jnp.bfloat16)
            ko_buf[rows, at] = dk[n + 2] * scale
            vo_buf[rows, at] = dv[n + 2]

    def send_out(buf, out, slot, h):
        cols = pl.ds(pl.multiple_of(core * half + h * HEAD_DIM, HEAD_DIM), HEAD_DIM)
        for b in range(2):
            remote(
                buf.at[pl.ds(b * tokens, tokens), lanes(h)],
                out.at[0, :, cols],
                os_sem.at[slot],
                o_sem.at[slot],
                homes[b],
            ).start()

    def finish(h):
        at = lanes(h)
        for got, own, done, out, sem, slot in (
            (kr_buf, ko_buf, kf_buf, dk_ref, kr_sem, 1),
            (vr_buf, vo_buf, vf_buf, dv_ref, vr_sem, 2),
        ):
            piece = got.at[:, at]
            remote(piece, piece, rs_sem.at[0], sem.at[h], partner).wait_recv()
            done[:, at] = (own[:, at] + got[:, at].astype(jnp.float32)).astype(jnp.bfloat16)
            send_out(done, out, slot, h)

    group = 2 * HEAD_DIM
    groups = half // group
    part = wg_ref.shape[1] * 8

    def group_rows(n):
        return pl.ds(pl.multiple_of(n * group, group), group)

    def columns_of(n, size):
        return pl.ds(pl.multiple_of(n * size, size), size)

    def f32(value):
        return value.astype(jnp.float32)

    def product(n):
        rows = group_rows(n)

        @pl.loop(0, 4)
        def _(i):
            cols = columns_of(i, part)
            p_buf[rows, cols] = mm(at_buf[rows, :], g_buf[:, cols], AB).astype(jnp.bfloat16)

        for slot, block in enumerate((x_pair[0], x_far)):
            remote(
                p_buf.at[rows, columns_of(block, part)],
                x1_buf.at[rows, pl.ds(slot * part, part)],
                px_sem.at[0],
                x1_sem.at[n],
                x_dev[0],
            ).start()

    def landed(ref, sem):
        remote(ref, ref, px_sem.at[0], sem, partner).wait_recv()

    def x_second(n):
        rows = group_rows(n)
        landed(x1_buf.at[rows], x1_sem.at[n])
        for slot, block in ((1, x_pair[1]), (0, x_at)):
            cols = pl.ds(slot * part, part)
            total = f32(p_buf[rows, columns_of(block, part)]) + f32(x1_buf[rows, cols])
            x1_buf[rows, cols] = total.astype(jnp.bfloat16)
            if slot == 1:
                remote(
                    x1_buf.at[rows, cols], x2_buf.at[rows], px_sem.at[1], x2_sem.at[n], x_dev[1]
                ).start()

    def y_first(n):
        rows = group_rows(n)
        landed(x2_buf.at[rows], x2_sem.at[n])
        total = f32(x1_buf[rows, pl.ds(0, part)]) + f32(x2_buf[rows, :])
        x2_buf[rows, :] = total.astype(jnp.bfloat16)
        for slot, block in enumerate((y_pair[0], y_far)):
            remote(
                x2_buf.at[rows, columns_of(block, 128)],
                y1_buf.at[rows, pl.ds(slot * 128, 128)],
                px_sem.at[2],
                y1_sem.at[n],
                y_dev[0],
            ).start()

    def y_second(n):
        rows = group_rows(n)
        landed(y1_buf.at[rows], y1_sem.at[n])
        for slot, block in ((1, y_pair[1]), (0, y_at)):
            cols = pl.ds(slot * 128, 128)
            total = f32(x2_buf[rows, columns_of(block, 128)]) + f32(y1_buf[rows, cols])
            y1_buf[rows, cols] = total.astype(jnp.bfloat16)
            if slot == 1:
                remote(
                    y1_buf.at[rows, cols], y2_buf.at[rows], px_sem.at[3], y2_sem.at[n], y_dev[1]
                ).start()

    def z_each(n, sent):
        rows = group_rows(n)
        owner = lax.div(n, groups // 2)
        slot_rows = group_rows(lax.rem(n, groups // 2))
        for b in range(2):
            own = (zl == core) & (owner == core) & (zh == b)
            copy = remote(
                y2_buf.at[rows],
                zr_buf.at[2 * zh + zl, slot_rows],
                px_sem.at[4],
                zr_sem.at[lax.rem(n, groups // 2)],
                device(col, b, core, owner),
            )

            @pl.when(jnp.logical_not(own))
            def _():
                if sent:
                    copy.wait_send()
                else:
                    copy.start()

            if not sent:

                @pl.when(own)
                def _():
                    zr_buf[2 * zh + zl, slot_rows, :] = y2_buf[rows, :]

    def z_send(n):
        rows = group_rows(n)
        landed(y2_buf.at[rows], y2_sem.at[n])
        total = f32(y1_buf[rows, pl.ds(0, 128)]) + f32(y2_buf[rows, :])
        y2_buf[rows, :] = total.astype(jnp.bfloat16)
        z_each(n, False)

    stages = (product, x_second, y_first, y_second, z_send)

    def reduce_step(t):
        for late, stage in enumerate(stages):

            @pl.when((t >= late) & (t - late < groups))
            def _():
                stage(t - late)

    @pl.loop(0, heads)
    def _(h):
        @pl.when(h + 1 < heads)
        def _():
            forward(h + 1)

        at = lanes(h)
        piece = q_buf.at[:, at]
        remote(piece, piece, zs_sem.at[2], qz_sem.at[h], partner).wait_recv()
        for buf, sem in ((k_buf, ky_sem), (v_buf, vy_sem)):
            piece = buf.at[halo_rows, at]
            remote(piece, piece, ys_sem.at[0], sem.at[h], partner).wait_recv()
        head(h)
        for src, dst, sem, slot in ((kh_buf, kr_buf, kr_sem, 0), (vh_buf, vr_buf, vr_sem, 1)):
            remote(
                src.at[:, at], dst.at[:, at], rs_sem.at[slot], sem.at[h], previous
            ).start()
        send_out(dq_buf, dq_ref, 0, h)

        @pl.when(h >= 2)
        def _():
            finish(h - 2)

        @pl.when(lax.rem(h, 2) == 1)
        def _():
            reduce_step(lax.div(h, 2))

    @pl.loop(groups, groups + len(stages) - 1)
    def _(t):
        @pl.when(t < groups + 2)
        def _():
            finish(t - groups + heads - 2)

        reduce_step(t)

    for n in range(groups // 2):
        rows = pl.ds(n * group, group)
        every = zr_buf.at[:, rows]
        some = zr_buf.at[pl.ds(0, 3), rows]

        @pl.when(zl == core)
        def _():
            landed(some, zr_sem.at[n])

        @pl.when(zl != core)
        def _():
            landed(every, zr_sem.at[n])

        total = f32(zr_buf[0, rows, :])
        for i in range(1, 4):
            total = total + f32(zr_buf[i, rows, :])
        wg_ref[rows, :] = jnp.where(zh == 0, total[:, :64], total[:, 64:])

    for ref, slot in ((k_ref, 0), (v_ref, 1), (q_ref, 2)):
        remote(ref, ref, zs_sem.at[slot], o_sem.at[0], partner).wait_send()
    remote(gm_buf, gm_buf, zs_sem.at[3], o_sem.at[0], partner).wait_send()
    for buf, slot in ((x1_buf, 0), (x2_buf, 1), (y1_buf, 2), (y2_buf, 3)):
        remote(buf, buf, px_sem.at[slot], o_sem.at[0], partner).wait_send()

    @pl.loop(0, groups)
    def _(n):
        z_each(n, True)


    @pl.when(core != zl)
    def _():
        w_send(partner).wait_send()

    @pl.when(zh == core)
    def _():
        for to in w_far:
            w_send(to).wait_send()

    g_swap.wait_send()
    for buf, slot in ((kr_buf, 0), (vr_buf, 1)):
        remote(buf, buf, ys_sem.at[slot], o_sem.at[0], partner).wait_send()
        remote(buf, buf, rs_sem.at[slot], o_sem.at[0], partner).wait_send()
    for buf, out, slot in ((dq_buf, dq_ref, 0), (kf_buf, dk_ref, 1), (vf_buf, dv_ref, 2)):
        remote(buf, buf, os_sem.at[slot], o_sem.at[0], partner).wait_send()
        remote(out, out, os_sem.at[slot], o_sem.at[slot], partner).wait_recv()


def per_device(queries, keys, values, out_grad, proj_weight, lengths):
    tokens, width = queries.shape[1:]
    half = width // 2
    heads = half // HEAD_DIM
    grad_width = out_grad.shape[2]
    groups = heads // 2
    any_space = pl.BlockSpec(memory_space=pl.ANY)
    dma = pltpu.SemaphoreType.DMA
    bf16 = jnp.bfloat16

    def vmem(*shape, dtype=bf16):
        return pltpu.VMEM(shape, dtype)

    pair = vmem(2 * tokens, half)
    outs = jax.ShapeDtypeStruct(queries.shape, bf16)
    weight_grad = jax.ShapeDtypeStruct(
        (width // lax.axis_size("dp"), grad_width // lax.axis_size("seq")), jnp.float32
    )
    return pl.pallas_call(
        attention_kernel,
        out_shape=(outs, outs, outs, weight_grad),
        in_specs=[any_space] * 5 + [pl.BlockSpec(memory_space=pltpu.SMEM)],
        out_specs=(any_space, any_space, any_space, pl.BlockSpec(memory_space=pltpu.VMEM)),
        scratch_shapes=[
            pair,
            vmem(4 * tokens, half),
            vmem(4 * tokens, half),
            vmem(2 * tokens, grad_width),
            vmem(half, grad_width),
            vmem(half, 2 * tokens),
            vmem(half, 2 * tokens),
            pair,
            pair,
            pair,
            pair,
            pair,
            vmem(2 * tokens, half, dtype=jnp.float32),
            vmem(2 * tokens, half, dtype=jnp.float32),
            pair,
            pair,
            vmem(tokens, grad_width),
            vmem(half, grad_width),
            vmem(half, grad_width // 2),
            vmem(half, grad_width // 4),
            vmem(half, grad_width // 8),
            vmem(half, grad_width // 16),
            vmem(4, half // 2, grad_width // 16),
            dma,
            dma((5,)),
            dma((groups,)),
            dma((groups,)),
            dma((groups,)),
            dma((groups,)),
            dma((groups // 2,)),
            dma((6,)),
            dma((heads,)),
            dma((heads,)),
            dma((heads,)),
            dma,
            dma,
            dma,
            dma,
            dma((2,)),
            dma((heads,)),
            dma((heads,)),
            dma((2,)),
            dma((heads,)),
            dma((heads,)),
            dma((3,)),
            dma((3,)),
        ],
        compiler_params=pltpu.CompilerParams(
            collective_id=0, has_side_effects=True, vmem_limit_bytes=66_000_000
        ),
        name="attention",
    )(queries, keys, values, out_grad, proj_weight, lengths)


def solution(mesh):
    placed = (
        P("dp", "seq", None),
        P("dp", "seq", None),
        P("dp", "seq", None),
        P("dp", "seq", None),
        P("dp", None),
        P("dp"),
    )
    return jax.shard_map(
        per_device,
        mesh=mesh,
        in_specs=placed,
        out_specs=(
            P("dp", "seq", None),
            P("dp", "seq", None),
            P("dp", "seq", None),
            P("dp", "seq"),
        ),
        check_vma=False,
    )
```

```python
import jax
import jax.numpy as jnp
from jax import lax
from jax.experimental import pallas as pl
from jax.experimental.pallas import tpu as pltpu
from jax.sharding import PartitionSpec as P

HEAD_DIM = 128
LOG2E = 1.4426950408889634
QUERY_LAG = 2
KEY_LAG = 4
AHEAD = 4
SUM_LAG = 2
MESH = pl.DeviceIdType.MESH

AB = (((1,), (0,)), ((), ()))
ABT = (((1,), (1,)), ((), ()))


def mm(left, right, dims):
    return lax.dot_general(left, right, dims, preferred_element_type=jnp.float32)


def attention_kernel(
    q_ref,
    k_ref,
    v_ref,
    g_ref,
    w_ref,
    len_ref,
    dq_ref,
    dk_ref,
    dv_ref,
    wg_ref,
    q_buf,
    k_buf,
    v_buf,
    g_buf,
    w_buf,
    do_buf,
    at_buf,
    dq_buf,
    kh_buf,
    vh_buf,
    kr_buf,
    vr_buf,
    ko_buf,
    vo_buf,
    kf_buf,
    vf_buf,
    gm_buf,
    p_buf,
    r1_buf,
    r2_buf,
    zs_buf,
    zr_buf,
    gl_sem,
    px_sem,
    r1_sem,
    r2_sem,
    zr_sem,
    zs_sem,
    kz_sem,
    vz_sem,
    qz_sem,
    g_sem,
    gx_sem,
    w_sem,
    wx_sem,
    wl_sem,
    ys_sem,
    ky_sem,
    vy_sem,
    rs_sem,
    kr_sem,
    vr_sem,
    os_sem,
    o_sem,
):
    seq = lax.axis_index("seq")
    dp = lax.axis_index("dp")
    columns = lax.axis_size("seq") // 2
    zh = lax.rem(seq, 2)
    col = lax.div(seq, 2)
    zl = lax.div(dp, 2)
    core = lax.rem(dp, 2)
    tokens = q_ref.shape[1]
    half = q_ref.shape[2] // 2
    heads = half // HEAD_DIM
    quarter = w_ref.shape[0]
    scale = HEAD_DIM ** (-0.5)

    def device(col_, zh_, zl_, core_):
        return (2 * col_ + zh_, 2 * zl_ + core_)

    targets = [device(col, core, 1 - zl, t) for t in range(2)]
    homes = [device(col, b, 1 - zl, zh) for b in range(2)]
    following = device(lax.rem(col + 1, columns), zh, zl, core)
    previous = device(lax.rem(col + columns - 1, columns), zh, zl, core)
    partner = device(col, zh, zl, 1 - core)

    g_local = pltpu.make_async_copy(g_ref.at[0], gm_buf, gl_sem)
    g_local.start()

    x_at = lax.div(col, 4)
    y_at = lax.rem(col, 4)

    def ring(at, step):
        return lax.rem(at + step + 4, 4)

    x_up, x_down = (device(4 * ring(x_at, i) + y_at, zh, zl, core) for i in (1, -1))
    y_up, y_down = (device(4 * x_at + ring(y_at, i), zh, zl, core) for i in (1, -1))

    barrier = pltpu.get_barrier_semaphore()
    greeted = [following, previous, x_up, x_down, y_up, y_down]
    for i in range(1, 8):
        greeted.append(
            device(
                col,
                1 - zh if i & 4 else zh,
                1 - zl if i & 2 else zl,
                1 - core if i & 1 else core,
            )
        )
    for other in greeted:
        pl.semaphore_signal(barrier, inc=1, device_id=other, device_id_type=MESH)
    with jax.named_scope("barrier"):
        pl.semaphore_wait(barrier, len(greeted))

    def remote(src, dst, send_sem, recv_sem, to):
        return pltpu.make_async_remote_copy(
            src_ref=src,
            dst_ref=dst,
            send_sem=send_sem,
            recv_sem=recv_sem,
            device_id=to,
            device_id_type=MESH,
        )

    def lanes(h):
        return pl.ds(pl.multiple_of(h * HEAD_DIM, HEAD_DIM), HEAD_DIM)

    my_rows = pl.ds(pl.multiple_of(zh * tokens, tokens), tokens)
    own_rows = pl.ds(2 * tokens, 2 * tokens)
    halo_rows = pl.ds(0, 2 * tokens)
    my_half = pl.ds(pl.multiple_of(core * half, half), half)

    def send_home(ref, buf, base, h, recv_sem, slot):
        rows = pl.ds(pl.multiple_of(base + zh * tokens, tokens), tokens)
        for t in range(2):
            src = pl.ds(pl.multiple_of(t * half + h * HEAD_DIM, HEAD_DIM), HEAD_DIM)
            remote(
                ref.at[0, :, src],
                buf.at[rows, lanes(h)],
                zs_sem.at[slot],
                recv_sem.at[h],
                targets[t],
            ).start()

    far = core != zl
    piece_rows = quarter // 8
    w_rows = pl.ds(pl.multiple_of(core * quarter, quarter), quarter)
    w_local = pltpu.make_async_copy(w_ref, w_buf.at[w_rows], wl_sem)
    w_swap = remote(w_ref, w_buf.at[w_rows], zs_sem.at[4], w_sem.at[2], partner)
    w_axes = ((x_at, x_down), (y_at, y_down))

    def w_piece(axis, j, at):
        first_row = j * quarter + axis * (quarter // 2) + at * piece_rows
        return w_buf.at[pl.ds(pl.multiple_of(first_row, piece_rows), piece_rows)]

    def w_source(axis):
        first_row = axis * (quarter // 2) + w_axes[axis][0] * piece_rows
        return w_ref.at[pl.ds(pl.multiple_of(first_row, piece_rows), piece_rows)]

    w_out = [
        remote(
            w_source(axis),
            w_piece(axis, core, w_axes[axis][0]),
            zs_sem.at[4],
            w_sem.at[axis],
            device(col, b, 1 - zl, zl),
        )
        for axis in range(2)
        for b in range(2)
    ]

    def w_hop(axis, step):
        at, down = w_axes[axis]
        pieces = [w_piece(axis, j, ring(at, step)) for j in range(2)]
        return [
            remote(piece, piece, wx_sem.at[6], wx_sem.at[2 * step + axis], down)
            for piece in pieces
        ]

    def w_wait(sem):
        pieces = w_buf.at[pl.ds(0, 2 * piece_rows)]
        with jax.named_scope("w_wait"):
            remote(pieces, pieces, zs_sem.at[4], sem, partner).wait_recv()

    def w_step(step):
        @pl.when(far)
        def _():
            for axis in range(2):
                w_wait(w_sem.at[axis] if step == 0 else wx_sem.at[2 * step - 2 + axis])
                if step < 3:
                    for copy in w_hop(axis, step):
                        copy.start()

    @pl.when(far)
    def _():
        w_swap.start()

    @pl.when(jnp.logical_not(far))
    def _():
        w_local.start()

    @pl.when(zh == core)
    def _():
        for copy in w_out:
            copy.start()

    def send_keys(h):
        send_home(k_ref, k_buf, 2 * tokens, h, kz_sem, 0)
        send_home(v_ref, v_buf, 2 * tokens, h, vz_sem, 1)

    def send_queries(h):
        send_home(q_ref, q_buf, 0, h, qz_sem, 2)

    g_parts = 4
    g_width = half // g_parts
    send_keys(0)
    g_local.wait()
    limit = len_ref[0] - seq * tokens
    live = lax.broadcasted_iota(jnp.int32, gm_buf.shape, 0) < limit
    gm_buf[...] = jnp.where(live, gm_buf[...], jnp.zeros_like(gm_buf))
    for i in range(g_parts):
        for t in range(2):
            cols = pl.ds(t * half + i * g_width, g_width)
            remote(
                gm_buf.at[:, cols], g_buf.at[my_rows, cols], zs_sem.at[3], g_sem.at[i], targets[t]
            ).start()
        if i + 1 < g_parts:
            send_keys(i + 1)
    send_queries(0)

    @pl.loop(g_parts, heads)
    def _(h):
        send_keys(h)
        for i in range(2):
            n = 2 * (h - g_parts) + 1 + i

            @pl.when(n < heads)
            def _():
                send_queries(n)

    def forward(h):
        for buf, got, sem, slot in (
            (k_buf, kz_sem, ky_sem, 0),
            (v_buf, vz_sem, vy_sem, 1),
        ):
            own = buf.at[own_rows, lanes(h)]
            with jax.named_scope("kv_wait"):
                remote(own, own, zs_sem.at[0], got.at[h], partner).wait_recv()
            remote(own, buf.at[halo_rows, lanes(h)], ys_sem.at[slot], sem.at[h], following).start()

    def g_piece(i):
        cols = pl.ds(pl.multiple_of(core * half + i * g_width, g_width), g_width)
        return g_buf.at[:, cols]

    def g_swap(i):
        return remote(g_piece(i), g_piece(i), zs_sem.at[5], gx_sem.at[i], partner)

    def g_exchange(i):
        with jax.named_scope("g_wait"):
            remote(g_piece(i), g_piece(i), zs_sem.at[3], g_sem.at[i], partner).wait_recv()
        g_swap(i).start()

    w_step(0)
    forward(0)
    w_step(1)
    g_exchange(0)
    forward(1)
    w_step(2)
    g_exchange(1)
    w_step(3)
    forward(2)
    g_exchange(2)
    forward(3)
    g_exchange(3)

    @pl.when(jnp.logical_not(far))
    def _():
        w_local.wait()
        remote(w_ref, w_ref, zs_sem.at[4], w_sem.at[2], partner).wait_recv()

    with jax.named_scope("gx_wait"):
        for i in range(g_parts):
            g_swap(i).wait_recv()

    with jax.named_scope("out_bwd"):

        @pl.loop(0, 2 * tokens // 256)
        def _(n):
            rows = pl.ds(pl.multiple_of(n * 256, 256), 256)
            do_buf[:, rows] = mm(w_buf[...], g_buf[rows, :], ABT).astype(jnp.bfloat16)

    first = jnp.where(col == 0, -1e30, 0.0).astype(jnp.float32)
    key_pos = lax.broadcasted_iota(jnp.int32, (tokens, tokens), 0)
    query_pos = lax.broadcasted_iota(jnp.int32, (tokens, tokens), 1)

    def head(h):
        at = lanes(h)
        feats = pl.ds(pl.multiple_of(h * HEAD_DIM, HEAD_DIM), HEAD_DIM)
        value_t = v_buf[:, at].T
        key_t = k_buf[:, at].T
        dk = [None] * 4
        dv = [None] * 4

        def add(total, block, term):
            total[block] = term if total[block] is None else total[block] + term

        for b in range(2):
            rows = slice(b * tokens, (b + 1) * tokens)
            q = q_buf[rows, at]
            do = do_buf[feats, rows]
            blocks = [b, b + 1, b + 2]
            tile = [slice(n * tokens, (n + 1) * tokens) for n in blocks]
            scores = []
            for j in range(3):
                s = mm(k_buf[tile[j], at], q, ABT)
                if blocks[j] < 2:
                    s = s + first
                if j == 2:
                    s = jnp.where(key_pos <= query_pos, s, -1e30)
                scores.append(s)
            top = scores[0].max(axis=0, keepdims=True)
            for s in scores[1:]:
                top = jnp.maximum(top, s.max(axis=0, keepdims=True))
            probs = [jnp.exp2((s - top) * (scale * LOG2E)) for s in scores]
            total = probs[0].sum(axis=0, keepdims=True)
            for p in probs[1:]:
                total = total + p.sum(axis=0, keepdims=True)
            inverse = 1.0 / total
            probs = [p * inverse for p in probs]
            attn = None
            for j in range(3):
                probs_b = probs[j].astype(jnp.bfloat16)
                term = mm(value_t[:, tile[j]], probs_b, AB)
                attn = term if attn is None else attn + term
                add(dv, blocks[j], mm(probs_b, do, ABT))
            attn = attn.astype(jnp.bfloat16)
            at_buf[feats, rows] = attn
            delta = jnp.sum(
                do.astype(jnp.float32) * attn.astype(jnp.float32), axis=0, keepdims=True
            )
            dq = None
            for j in range(3):
                grad = mm(v_buf[tile[j], at], do, AB)
                sg = (probs[j] * (grad - delta)).astype(jnp.bfloat16)
                term = mm(key_t[:, tile[j]], sg, AB)
                dq = term if dq is None else dq + term
                add(dk, blocks[j], mm(sg, q, AB))
            dq_buf[rows, at] = (dq * scale).T.astype(jnp.bfloat16)
        for n in range(2):
            rows = slice(n * tokens, (n + 1) * tokens)
            kh_buf[rows, at] = (dk[n] * scale).astype(jnp.bfloat16)
            vh_buf[rows, at] = dv[n].astype(jnp.bfloat16)
            ko_buf[rows, at] = dk[n + 2] * scale
            vo_buf[rows, at] = dv[n + 2]

    def send_out(buf, out, slot, h):
        cols = pl.ds(pl.multiple_of(core * half + h * HEAD_DIM, HEAD_DIM), HEAD_DIM)
        for b in range(2):
            remote(
                buf.at[pl.ds(b * tokens, tokens), lanes(h)],
                out.at[0, :, cols],
                os_sem.at[slot],
                o_sem.at[slot],
                homes[b],
            ).start()

    def finish(h):
        at = lanes(h)
        for got, own, done, out, sem, slot in (
            (kr_buf, ko_buf, kf_buf, dk_ref, kr_sem, 1),
            (vr_buf, vo_buf, vf_buf, dv_ref, vr_sem, 2),
        ):
            piece = got.at[:, at]
            with jax.named_scope("back_wait"):
                remote(piece, piece, rs_sem.at[0], sem.at[h], partner).wait_recv()
            done[:, at] = (own[:, at] + got[:, at].astype(jnp.float32)).astype(jnp.bfloat16)
            send_out(done, out, slot, h)

    def give_back(t):
        for lag, task in ((QUERY_LAG, lambda h: send_out(dq_buf, dq_ref, 0, h)), (KEY_LAG, finish)):

            @pl.when((t >= lag) & (t - lag < heads))
            def _():
                task(t - lag)

    group = 2 * HEAD_DIM
    groups = half // group
    wide = 128
    part = 4 * wide
    along_x = core == 0
    outer_at = jnp.where(along_x, x_at, y_at)
    inner_at = jnp.where(along_x, y_at, x_at)

    def device_of(first, second):
        return tuple(jnp.where(along_x, a, b) for a, b in zip(first, second))

    outer_up = device_of(x_up, y_up)
    inner_up = device_of(y_up, x_up)

    def group_rows(n):
        return pl.ds(pl.multiple_of(n * group, group), group)

    def columns_of(n, size):
        return pl.ds(pl.multiple_of(n * size, size), size)

    def f32(value):
        return value.astype(jnp.float32)

    def landed(ref, sem):
        with jax.named_scope("sum_wait"):
            remote(ref, ref, px_sem.at[0], sem, partner).wait_recv()

    def outer_send(n, step, src):
        remote(
            src, r1_buf.at[step, group_rows(n)], px_sem.at[step], r1_sem.at[step, n], outer_up
        ).start()

    def inner_send(n, step, src):
        remote(
            src, r2_buf.at[step, group_rows(n)], px_sem.at[3 + step], r2_sem.at[step, n], inner_up
        ).start()

    def product(n):
        rows = group_rows(n)

        @pl.loop(0, 4)
        def _(x):
            term = mm(at_buf[rows, :], g_buf[:, columns_of(x, part)], AB).astype(jnp.bfloat16)
            for y in range(4):
                place = jnp.where(along_x, 4 * x + y, 4 * y + x)
                p_buf[rows, columns_of(place, wide)] = term[:, y * wide : (y + 1) * wide]

        outer_send(n, 0, p_buf.at[rows, columns_of(ring(outer_at, -1), part)])

    def outer(step, n):
        rows = group_rows(n)
        landed(r1_buf.at[step, rows], r1_sem.at[step, n])
        cols = columns_of(ring(outer_at, -2 - step), part)
        total = f32(p_buf[rows, cols]) + f32(r1_buf[step, rows, :])
        r1_buf[step, rows, :] = total.astype(jnp.bfloat16)
        if step < 2:
            outer_send(n, step + 1, r1_buf.at[step, rows])
        else:
            inner_send(n, 0, r1_buf.at[2, rows, columns_of(ring(inner_at, -1), wide)])

    def inner(step, n):
        rows = group_rows(n)
        landed(r2_buf.at[step, rows], r2_sem.at[step, n])
        cols = columns_of(ring(inner_at, -2 - step), wide)
        total = f32(r1_buf[2, rows, cols]) + f32(r2_buf[step, rows, :])
        if step < 2:
            r2_buf[step, rows, :] = total.astype(jnp.bfloat16)
            inner_send(n, step + 1, r2_buf.at[step, rows])
        else:
            z_send(n, total)

    short = group // 2

    def packed_rows(n):
        return pl.ds(pl.multiple_of(n * short, short), short)

    def z_each(n, sent):
        owner = lax.div(n, groups // 2)
        slot_rows = packed_rows(lax.rem(n, groups // 2))
        for b in range(2):
            own = (zl == core) & (owner == core) & (zh == b)
            copy = remote(
                zs_buf.at[b, packed_rows(n)],
                zr_buf.at[2 * zh + zl, slot_rows],
                px_sem.at[6],
                zr_sem.at[lax.rem(n, groups // 2)],
                device(col, b, core, owner),
            )

            @pl.when(jnp.logical_not(own))
            def _():
                if sent:
                    copy.wait_send()
                else:
                    copy.start()

            if not sent:

                @pl.when(own)
                def _():
                    zr_buf[2 * zh + zl, slot_rows, :] = zs_buf[b, packed_rows(n), :]

    def z_send(n, total):
        upper, lower = total[:short], total[short:]
        left = lax.broadcasted_iota(jnp.int32, upper.shape, 1) < wide // 2
        for b, packed in enumerate(
            (
                jnp.where(left, upper, pltpu.roll(lower, wide // 2, 1)),
                jnp.where(left, pltpu.roll(upper, wide // 2, 1), lower),
            )
        ):
            zs_buf[b, packed_rows(n), :] = packed.astype(jnp.bfloat16)
        z_each(n, False)

    stages = [product]
    stages += [lambda n, step=step: outer(step, n) for step in range(3)]
    stages += [lambda n, step=step: inner(step, n) for step in range(3)]

    def reduce_step(t):
        for late, stage in enumerate(stages):
            n = t - 1 - late - (SUM_LAG if late else 0)

            @pl.when((n >= 0) & (lax.rem(n + 2 * heads, 2) == 0) & (n < 2 * groups))
            def _():
                with jax.named_scope(f"stage{late}"):
                    stage(lax.div(n, 2))

    @pl.loop(0, heads)
    def _(h):
        @pl.when(h + AHEAD < heads)
        def _():
            forward(h + AHEAD)

        at = lanes(h)
        piece = q_buf.at[:, at]
        with jax.named_scope("q_wait"):
            remote(piece, piece, zs_sem.at[2], qz_sem.at[h], partner).wait_recv()
        for buf, sem in ((k_buf, ky_sem), (v_buf, vy_sem)):
            piece = buf.at[halo_rows, at]
            with jax.named_scope("halo_wait"):
                remote(piece, piece, ys_sem.at[0], sem.at[h], partner).wait_recv()
        with jax.named_scope("head"):
            head(h)
        for src, dst, sem, slot in ((kh_buf, kr_buf, kr_sem, 0), (vh_buf, vr_buf, vr_sem, 1)):
            remote(
                src.at[:, at], dst.at[:, at], rs_sem.at[slot], sem.at[h], previous
            ).start()
        give_back(h)

        reduce_step(h)

    @pl.loop(heads, heads + len(stages) + SUM_LAG)
    def _(t):
        give_back(t)
        reduce_step(t)

    for n in range(groups // 2):
        rows = pl.ds(n * short, short)
        every = zr_buf.at[:, rows]
        some = zr_buf.at[pl.ds(0, 3), rows]

        @pl.when(zl == core)
        def _():
            landed(some, zr_sem.at[n])

        @pl.when(zl != core)
        def _():
            landed(every, zr_sem.at[n])

        total = f32(zr_buf[0, rows, :])
        for i in range(1, 4):
            total = total + f32(zr_buf[i, rows, :])
        wg_ref[pl.ds(n * group, short), :] = total[:, : wide // 2]
        wg_ref[pl.ds(n * group + short, short), :] = total[:, wide // 2 :]

    with jax.named_scope("drain"):
        for ref, slot in ((k_ref, 0), (v_ref, 1), (q_ref, 2)):
            remote(ref, ref, zs_sem.at[slot], o_sem.at[0], partner).wait_send()
        remote(gm_buf, gm_buf, zs_sem.at[3], o_sem.at[0], partner).wait_send()
        for step in range(3):
            for buf, slot in ((r1_buf, step), (r2_buf, 3 + step)):
                remote(buf.at[0], buf.at[0], px_sem.at[slot], o_sem.at[0], partner).wait_send()

        @pl.loop(0, groups)
        def _(n):
            z_each(n, True)


        @pl.when(far)
        def _():
            w_swap.wait_send()
            for axis in range(2):
                for step in range(3):
                    for copy in w_hop(axis, step):
                        copy.wait_send()

        @pl.when(zh == core)
        def _():
            for copy in w_out:
                copy.wait_send()

        for i in range(g_parts):
            g_swap(i).wait_send()
        for buf, slot in ((kr_buf, 0), (vr_buf, 1)):
            remote(buf, buf, ys_sem.at[slot], o_sem.at[0], partner).wait_send()
            remote(buf, buf, rs_sem.at[slot], o_sem.at[0], partner).wait_send()
        for buf, out, slot in ((dq_buf, dq_ref, 0), (kf_buf, dk_ref, 1), (vf_buf, dv_ref, 2)):
            remote(buf, buf, os_sem.at[slot], o_sem.at[0], partner).wait_send()
            remote(out, out, os_sem.at[slot], o_sem.at[slot], partner).wait_recv()


def per_device(queries, keys, values, out_grad, proj_weight, lengths):
    tokens, width = queries.shape[1:]
    half = width // 2
    heads = half // HEAD_DIM
    grad_width = out_grad.shape[2]
    groups = heads // 2
    any_space = pl.BlockSpec(memory_space=pl.ANY)
    dma = pltpu.SemaphoreType.DMA
    bf16 = jnp.bfloat16

    def vmem(*shape, dtype=bf16):
        return pltpu.VMEM(shape, dtype)

    pair = vmem(2 * tokens, half)
    outs = jax.ShapeDtypeStruct(queries.shape, bf16)
    weight_grad = jax.ShapeDtypeStruct(
        (width // lax.axis_size("dp"), grad_width // lax.axis_size("seq")), jnp.float32
    )
    return pl.pallas_call(
        attention_kernel,
        out_shape=(outs, outs, outs, weight_grad),
        in_specs=[any_space] * 5 + [pl.BlockSpec(memory_space=pltpu.SMEM)],
        out_specs=(any_space, any_space, any_space, pl.BlockSpec(memory_space=pltpu.VMEM)),
        scratch_shapes=[
            pair,
            vmem(4 * tokens, half),
            vmem(4 * tokens, half),
            vmem(2 * tokens, grad_width),
            vmem(half, grad_width),
            vmem(half, 2 * tokens),
            vmem(half, 2 * tokens),
            pair,
            pair,
            pair,
            pair,
            pair,
            vmem(2 * tokens, half, dtype=jnp.float32),
            vmem(2 * tokens, half, dtype=jnp.float32),
            pair,
            pair,
            vmem(tokens, grad_width),
            vmem(half, grad_width),
            vmem(3, half, grad_width // 4),
            vmem(3, half, grad_width // 16),
            vmem(2, half // 2, grad_width // 16),
            vmem(4, half // 4, grad_width // 16),
            dma,
            dma((7,)),
            dma((3, groups)),
            dma((3, groups)),
            dma((groups // 2,)),
            dma((6,)),
            dma((heads,)),
            dma((heads,)),
            dma((heads,)),
            dma((4,)),
            dma((4,)),
            dma((3,)),
            dma((7,)),
            dma,
            dma((2,)),
            dma((heads,)),
            dma((heads,)),
            dma((2,)),
            dma((heads,)),
            dma((heads,)),
            dma((3,)),
            dma((3,)),
        ],
        compiler_params=pltpu.CompilerParams(
            collective_id=0, has_side_effects=True, vmem_limit_bytes=66_000_000
        ),
        name="attention",
    )(queries, keys, values, out_grad, proj_weight, lengths)


def solution(mesh):
    placed = (
        P("dp", "seq", None),
        P("dp", "seq", None),
        P("dp", "seq", None),
        P("dp", "seq", None),
        P("dp", None),
        P("dp"),
    )
    return jax.shard_map(
        per_device,
        mesh=mesh,
        in_specs=placed,
        out_specs=(
            P("dp", "seq", None),
            P("dp", "seq", None),
            P("dp", "seq", None),
            P("dp", "seq"),
        ),
        check_vma=False,
    )
```

```python
import functools

import jax
import jax.numpy as jnp
from jax import lax
from jax.experimental import pallas as pl
from jax.experimental.pallas import tpu as pltpu
from jax.sharding import PartitionSpec as P

HEAD_DIM = 128
LOG2E = 1.4426950408889634
QUERY_LAG = 2
KEY_LAG = 4
AHEAD = 4
COPY_ROWS = 96
PRODUCTS = (1, 3, 5, 7)
SUMS = (3, 5, 6, 7)
MESH = pl.DeviceIdType.MESH

AB = (((1,), (0,)), ((), ()))
ABT = (((1,), (1,)), ((), ()))


def mm(left, right, dims):
    return lax.dot_general(left, right, dims, preferred_element_type=jnp.float32)


def attention_kernel(
    q_ref,
    k_ref,
    v_ref,
    g_ref,
    w_ref,
    len_ref,
    dq_ref,
    dk_ref,
    dv_ref,
    wg_ref,
    q_buf,
    k_buf,
    v_buf,
    g_buf,
    w_buf,
    do_buf,
    at_buf,
    dq_buf,
    kh_buf,
    vh_buf,
    kr_buf,
    vr_buf,
    ko_buf,
    vo_buf,
    kf_buf,
    vf_buf,
    gm_buf,
    p_buf,
    r1_buf,
    r2_buf,
    zs_buf,
    zr_buf,
    gl_sem,
    px_sem,
    r1_sem,
    r2_sem,
    zr_sem,
    zs_sem,
    kz_sem,
    vz_sem,
    qz_sem,
    g_sem,
    gx_sem,
    w_sem,
    wx_sem,
    wl_sem,
    ys_sem,
    ky_sem,
    vy_sem,
    rs_sem,
    kr_sem,
    vr_sem,
    os_sem,
    o_sem,
):
    seq = lax.axis_index("seq")
    dp = lax.axis_index("dp")
    columns = lax.axis_size("seq") // 2
    zh = lax.rem(seq, 2)
    col = lax.div(seq, 2)
    zl = lax.div(dp, 2)
    core = lax.rem(dp, 2)
    tokens = q_ref.shape[1]
    half = q_ref.shape[2] // 2
    heads = half // HEAD_DIM
    quarter = w_ref.shape[0]
    scale = HEAD_DIM ** (-0.5)

    def device(col_, zh_, zl_, core_):
        return (2 * col_ + zh_, 2 * zl_ + core_)

    targets = [device(col, core, 1 - zl, t) for t in range(2)]
    homes = [device(col, b, 1 - zl, zh) for b in range(2)]
    following = device(lax.rem(col + 1, columns), zh, zl, core)
    previous = device(lax.rem(col + columns - 1, columns), zh, zl, core)
    partner = device(col, zh, zl, 1 - core)

    g_local = pltpu.make_async_copy(g_ref.at[0], gm_buf, gl_sem)
    g_local.start()

    x_at = lax.div(col, 4)
    y_at = lax.rem(col, 4)

    def ring(at, step):
        return lax.rem(at + step + 4, 4)

    x_up, x_down = (device(4 * ring(x_at, i) + y_at, zh, zl, core) for i in (1, -1))
    y_up, y_down = (device(4 * x_at + ring(y_at, i), zh, zl, core) for i in (1, -1))

    barrier = pltpu.get_barrier_semaphore()
    greeted = [following, previous, x_up, x_down, y_up, y_down]
    for i in range(1, 8):
        greeted.append(
            device(
                col,
                1 - zh if i & 4 else zh,
                1 - zl if i & 2 else zl,
                1 - core if i & 1 else core,
            )
        )
    for other in greeted:
        pl.semaphore_signal(barrier, inc=1, device_id=other, device_id_type=MESH)
    with jax.named_scope("barrier"):
        pl.semaphore_wait(barrier, len(greeted))

    def remote(src, dst, send_sem, recv_sem, to):
        return pltpu.make_async_remote_copy(
            src_ref=src,
            dst_ref=dst,
            send_sem=send_sem,
            recv_sem=recv_sem,
            device_id=to,
            device_id_type=MESH,
        )

    def lanes(h):
        return pl.ds(pl.multiple_of(h * HEAD_DIM, HEAD_DIM), HEAD_DIM)

    my_rows = pl.ds(pl.multiple_of(zh * tokens, tokens), tokens)
    own_rows = pl.ds(2 * tokens, 2 * tokens)
    halo_rows = pl.ds(0, 2 * tokens)
    my_half = pl.ds(pl.multiple_of(core * half, half), half)

    def send_home(ref, buf, base, h, recv_sem, slot):
        rows = pl.ds(pl.multiple_of(base + zh * tokens, tokens), tokens)
        for t in range(2):
            src = pl.ds(pl.multiple_of(t * half + h * HEAD_DIM, HEAD_DIM), HEAD_DIM)
            remote(
                ref.at[0, :, src],
                buf.at[rows, lanes(h)],
                zs_sem.at[slot],
                recv_sem.at[h],
                targets[t],
            ).start()

    far = core != zl
    piece_rows = quarter // 8
    w_rows = pl.ds(pl.multiple_of(core * quarter, quarter), quarter)
    w_local = pltpu.make_async_copy(w_ref, w_buf.at[w_rows], wl_sem)
    w_swap = remote(w_ref, w_buf.at[w_rows], zs_sem.at[4], w_sem.at[2], partner)
    w_axes = ((x_at, x_down), (y_at, y_down))

    def w_piece(axis, j, at):
        first_row = j * quarter + axis * (quarter // 2) + at * piece_rows
        return w_buf.at[pl.ds(pl.multiple_of(first_row, piece_rows), piece_rows)]

    def w_source(axis):
        first_row = axis * (quarter // 2) + w_axes[axis][0] * piece_rows
        return w_ref.at[pl.ds(pl.multiple_of(first_row, piece_rows), piece_rows)]

    w_out = [
        remote(
            w_source(axis),
            w_piece(axis, core, w_axes[axis][0]),
            zs_sem.at[4],
            w_sem.at[axis],
            device(col, b, 1 - zl, zl),
        )
        for axis in range(2)
        for b in range(2)
    ]

    def w_hop(axis, step):
        at, down = w_axes[axis]
        pieces = [w_piece(axis, j, ring(at, step)) for j in range(2)]
        return [
            remote(piece, piece, wx_sem.at[6], wx_sem.at[2 * step + axis], down)
            for piece in pieces
        ]

    def w_wait(sem):
        pieces = w_buf.at[pl.ds(0, 2 * piece_rows)]
        with jax.named_scope("w_wait"):
            remote(pieces, pieces, zs_sem.at[4], sem, partner).wait_recv()

    def w_step(step):
        @pl.when(far)
        def _():
            for axis in range(2):
                w_wait(w_sem.at[axis] if step == 0 else wx_sem.at[2 * step - 2 + axis])
                if step < 3:
                    for copy in w_hop(axis, step):
                        copy.start()

    @pl.when(far)
    def _():
        w_swap.start()

    @pl.when(jnp.logical_not(far))
    def _():
        w_local.start()

    @pl.when(zh == core)
    def _():
        for copy in w_out:
            copy.start()

    def send_keys(h):
        send_home(k_ref, k_buf, 2 * tokens, h, kz_sem, 0)
        send_home(v_ref, v_buf, 2 * tokens, h, vz_sem, 1)

    def send_queries(h):
        send_home(q_ref, q_buf, 0, h, qz_sem, 2)

    g_parts = 4
    g_width = half // g_parts
    send_keys(0)
    g_local.wait()
    limit = len_ref[0] - seq * tokens
    live = lax.broadcasted_iota(jnp.int32, gm_buf.shape, 0) < limit
    gm_buf[...] = jnp.where(live, gm_buf[...], jnp.zeros_like(gm_buf))
    for i in range(g_parts):
        for t in range(2):
            cols = pl.ds(t * half + i * g_width, g_width)
            remote(
                gm_buf.at[:, cols], g_buf.at[my_rows, cols], zs_sem.at[3], g_sem.at[i], targets[t]
            ).start()
        if i + 1 < g_parts:
            send_keys(i + 1)
    send_queries(0)

    @pl.loop(g_parts, heads)
    def _(h):
        send_keys(h)
        for i in range(2):
            n = 2 * (h - g_parts) + 1 + i

            @pl.when(n < heads)
            def _():
                send_queries(n)

    def forward(h):
        for buf, got, sem, slot in (
            (k_buf, kz_sem, ky_sem, 0),
            (v_buf, vz_sem, vy_sem, 1),
        ):
            own = buf.at[own_rows, lanes(h)]
            with jax.named_scope("kv_wait"):
                remote(own, own, zs_sem.at[0], got.at[h], partner).wait_recv()
            remote(own, buf.at[halo_rows, lanes(h)], ys_sem.at[slot], sem.at[h], following).start()

    def g_piece(i):
        cols = pl.ds(pl.multiple_of(core * half + i * g_width, g_width), g_width)
        return g_buf.at[:, cols]

    def g_swap(i):
        return remote(g_piece(i), g_piece(i), zs_sem.at[5], gx_sem.at[i], partner)

    def g_exchange(i):
        with jax.named_scope("g_wait"):
            remote(g_piece(i), g_piece(i), zs_sem.at[3], g_sem.at[i], partner).wait_recv()
        g_swap(i).start()

    w_step(0)
    forward(0)
    w_step(1)
    g_exchange(0)
    forward(1)
    w_step(2)
    g_exchange(1)
    w_step(3)
    forward(2)
    g_exchange(2)
    forward(3)
    g_exchange(3)

    @pl.when(jnp.logical_not(far))
    def _():
        w_local.wait()
        remote(w_ref, w_ref, zs_sem.at[4], w_sem.at[2], partner).wait_recv()

    with jax.named_scope("gx_wait"):
        for i in range(g_parts):
            g_swap(i).wait_recv()

    with jax.named_scope("out_bwd"):

        @pl.loop(0, 2 * tokens // 256)
        def _(n):
            rows = pl.ds(pl.multiple_of(n * 256, 256), 256)
            do_buf[:, rows] = mm(w_buf[...], g_buf[rows, :], ABT).astype(jnp.bfloat16)

    first = jnp.where(col == 0, -1e30, 0.0).astype(jnp.float32)
    key_pos = lax.broadcasted_iota(jnp.int32, (tokens, tokens), 0)
    query_pos = lax.broadcasted_iota(jnp.int32, (tokens, tokens), 1)

    def head(h):
        at = lanes(h)
        feats = pl.ds(pl.multiple_of(h * HEAD_DIM, HEAD_DIM), HEAD_DIM)
        value_t = v_buf[:, at].T
        key_t = k_buf[:, at].T
        dk = [None] * 4
        dv = [None] * 4

        def add(total, block, term):
            total[block] = term if total[block] is None else total[block] + term

        for b in range(2):
            rows = slice(b * tokens, (b + 1) * tokens)
            q = q_buf[rows, at]
            do = do_buf[feats, rows]
            blocks = [b, b + 1, b + 2]
            tile = [slice(n * tokens, (n + 1) * tokens) for n in blocks]
            scores = []
            for j in range(3):
                s = mm(k_buf[tile[j], at], q, ABT)
                if blocks[j] < 2:
                    s = s + first
                if j == 2:
                    s = jnp.where(key_pos <= query_pos, s, -1e30)
                scores.append(s)
            top = scores[0].max(axis=0, keepdims=True)
            for s in scores[1:]:
                top = jnp.maximum(top, s.max(axis=0, keepdims=True))
            probs = [jnp.exp2((s - top) * (scale * LOG2E)) for s in scores]
            total = probs[0].sum(axis=0, keepdims=True)
            for p in probs[1:]:
                total = total + p.sum(axis=0, keepdims=True)
            inverse = 1.0 / total
            probs = [p * inverse for p in probs]
            attn = None
            for j in range(3):
                probs_b = probs[j].astype(jnp.bfloat16)
                term = mm(value_t[:, tile[j]], probs_b, AB)
                attn = term if attn is None else attn + term
                add(dv, blocks[j], mm(probs_b, do, ABT))
            attn = attn.astype(jnp.bfloat16)
            at_buf[feats, rows] = attn
            delta = jnp.sum(
                do.astype(jnp.float32) * attn.astype(jnp.float32), axis=0, keepdims=True
            )
            dq = None
            for j in range(3):
                grad = mm(v_buf[tile[j], at], do, AB)
                sg = (probs[j] * (grad - delta)).astype(jnp.bfloat16)
                term = mm(key_t[:, tile[j]], sg, AB)
                dq = term if dq is None else dq + term
                add(dk, blocks[j], mm(sg, q, AB))
            dq_buf[rows, at] = (dq * scale).T.astype(jnp.bfloat16)
        for n in range(2):
            rows = slice(n * tokens, (n + 1) * tokens)
            kh_buf[rows, at] = (dk[n] * scale).astype(jnp.bfloat16)
            vh_buf[rows, at] = dv[n].astype(jnp.bfloat16)
            ko_buf[rows, at] = dk[n + 2] * scale
            vo_buf[rows, at] = dv[n + 2]

    def send_out(buf, out, slot, h):
        cols = pl.ds(pl.multiple_of(core * half + h * HEAD_DIM, HEAD_DIM), HEAD_DIM)
        for b in range(2):
            remote(
                buf.at[pl.ds(b * tokens, tokens), lanes(h)],
                out.at[0, :, cols],
                os_sem.at[slot],
                o_sem.at[slot],
                homes[b],
            ).start()

    def finish(h):
        at = lanes(h)
        for got, own, done, out, sem, slot in (
            (kr_buf, ko_buf, kf_buf, dk_ref, kr_sem, 1),
            (vr_buf, vo_buf, vf_buf, dv_ref, vr_sem, 2),
        ):
            piece = got.at[:, at]
            with jax.named_scope("back_wait"):
                remote(piece, piece, rs_sem.at[0], sem.at[h], partner).wait_recv()
            done[:, at] = (own[:, at] + got[:, at].astype(jnp.float32)).astype(jnp.bfloat16)
            send_out(done, out, slot, h)

    def give_back(t):
        for lag, task in ((QUERY_LAG, lambda h: send_out(dq_buf, dq_ref, 0, h)), (KEY_LAG, finish)):

            @pl.when((t >= lag) & (t - lag < heads))
            def _():
                task(t - lag)

    group = 2 * HEAD_DIM
    groups = half // group
    wide = 128
    part = 4 * wide
    along_x = core == 0
    outer_at = jnp.where(along_x, x_at, y_at)
    inner_at = jnp.where(along_x, y_at, x_at)

    def device_of(first, second):
        return tuple(jnp.where(along_x, a, b) for a, b in zip(first, second))

    outer_up = device_of(x_up, y_up)
    inner_up = device_of(y_up, x_up)

    def group_rows(n):
        return pl.ds(pl.multiple_of(n * group, group), group)

    def columns_of(n, size):
        return pl.ds(pl.multiple_of(n * size, size), size)

    def f32(value):
        return value.astype(jnp.float32)

    def landed(ref, sem):
        with jax.named_scope("sum_wait"):
            remote(ref, ref, px_sem.at[0], sem, partner).wait_recv()

    def outer_send(n, step, src):
        remote(
            src, r1_buf.at[step, group_rows(n)], px_sem.at[step], r1_sem.at[step, n], outer_up
        ).start()

    def inner_send(n, step, src):
        remote(
            src, r2_buf.at[step, group_rows(n)], px_sem.at[3 + step], r2_sem.at[step, n], inner_up
        ).start()

    def product(n):
        rows = group_rows(n)

        @pl.loop(0, 4)
        def _(x):
            term = mm(at_buf[rows, :], g_buf[:, columns_of(x, part)], AB).astype(jnp.bfloat16)
            for y in range(4):
                place = jnp.where(along_x, 4 * x + y, 4 * y + x)
                p_buf[rows, columns_of(place, wide)] = term[:, y * wide : (y + 1) * wide]

        outer_send(n, 0, p_buf.at[rows, columns_of(ring(outer_at, -1), part)])

    def outer(step, n):
        rows = group_rows(n)
        landed(r1_buf.at[step, rows], r1_sem.at[step, n])
        cols = columns_of(ring(outer_at, -2 - step), part)
        total = f32(p_buf[rows, cols]) + f32(r1_buf[step, rows, :])
        r1_buf[step, rows, :] = total.astype(jnp.bfloat16)
        if step < 2:
            outer_send(n, step + 1, r1_buf.at[step, rows])
        else:
            inner_send(n, 0, r1_buf.at[2, rows, columns_of(ring(inner_at, -1), wide)])

    def inner(step, n):
        rows = group_rows(n)
        landed(r2_buf.at[step, rows], r2_sem.at[step, n])
        cols = columns_of(ring(inner_at, -2 - step), wide)
        total = f32(r1_buf[2, rows, cols]) + f32(r2_buf[step, rows, :])
        if step < 2:
            r2_buf[step, rows, :] = total.astype(jnp.bfloat16)
            inner_send(n, step + 1, r2_buf.at[step, rows])
        else:
            z_send(n, total)

    short = group // 2

    def packed_rows(n):
        return pl.ds(pl.multiple_of(n * short, short), short)

    def z_each(n, sent):
        owner = lax.div(n, groups // 2)
        slot_rows = packed_rows(lax.rem(n, groups // 2))
        for b in range(2):
            own = (zl == core) & (owner == core) & (zh == b)
            copy = remote(
                zs_buf.at[b, packed_rows(n)],
                zr_buf.at[2 * zh + zl, slot_rows],
                px_sem.at[6],
                zr_sem.at[lax.rem(n, groups // 2)],
                device(col, b, core, owner),
            )

            @pl.when(jnp.logical_not(own))
            def _():
                if sent:
                    copy.wait_send()
                else:
                    copy.start()

            if not sent:

                @pl.when(own)
                def _():
                    zr_buf[2 * zh + zl, slot_rows, :] = zs_buf[b, packed_rows(n), :]

    def z_send(n, total):
        upper, lower = total[:short], total[short:]
        left = lax.broadcasted_iota(jnp.int32, upper.shape, 1) < wide // 2
        for b, packed in enumerate(
            (
                jnp.where(left, upper, pltpu.roll(lower, wide // 2, 1)),
                jnp.where(left, pltpu.roll(upper, wide // 2, 1), lower),
            )
        ):
            zs_buf[b, packed_rows(n), :] = packed.astype(jnp.bfloat16)
        z_each(n, False)

    stages = [product]
    stages += [lambda n, step=step: outer(step, n) for step in range(3)]
    stages += [lambda n, step=step: inner(step, n) for step in range(3)]

    def reduce_step(t):
        for late, stage in enumerate(stages):
            times = SUMS if late else PRODUCTS
            due = functools.reduce(jnp.logical_or, [t - late == time for time in times])
            n = sum((t - late > time).astype(jnp.int32) for time in times)

            @pl.when(due)
            def _():
                with jax.named_scope(f"stage{late}"):
                    stage(n)

    @pl.loop(0, heads)
    def _(h):
        @pl.when(h + AHEAD < heads)
        def _():
            forward(h + AHEAD)

        at = lanes(h)
        piece = q_buf.at[:, at]
        with jax.named_scope("q_wait"):
            remote(piece, piece, zs_sem.at[2], qz_sem.at[h], partner).wait_recv()
        for buf, sem in ((k_buf, ky_sem), (v_buf, vy_sem)):
            piece = buf.at[halo_rows, at]
            with jax.named_scope("halo_wait"):
                remote(piece, piece, ys_sem.at[0], sem.at[h], partner).wait_recv()
        with jax.named_scope("head"):
            head(h)
        for src, dst, sem, slot in ((kh_buf, kr_buf, kr_sem, 0), (vh_buf, vr_buf, vr_sem, 1)):
            remote(
                src.at[:, at], dst.at[:, at], rs_sem.at[slot], sem.at[h], previous
            ).start()
        give_back(h)

        reduce_step(h)

    @pl.loop(heads, heads + max(KEY_LAG, SUMS[-1] + len(stages) - heads))
    def _(t):
        give_back(t)
        reduce_step(t)

    for n in range(groups // 2):
        rows = pl.ds(n * short, short)
        every = zr_buf.at[:, rows]
        some = zr_buf.at[pl.ds(0, 3), rows]

        @pl.when(zl == core)
        def _():
            landed(some, zr_sem.at[n])

        @pl.when(zl != core)
        def _():
            landed(every, zr_sem.at[n])

        total = f32(zr_buf[0, rows, :])
        for i in range(1, 4):
            total = total + f32(zr_buf[i, rows, :])
        turned = total.T
        wg_ref[:, pl.ds(n * group, short)] = turned[: wide // 2]
        wg_ref[:, pl.ds(n * group + short, short)] = turned[wide // 2 :]

    with jax.named_scope("drain"):
        for ref, slot in ((k_ref, 0), (v_ref, 1), (q_ref, 2)):
            remote(ref, ref, zs_sem.at[slot], o_sem.at[0], partner).wait_send()
        remote(gm_buf, gm_buf, zs_sem.at[3], o_sem.at[0], partner).wait_send()
        for step in range(3):
            for buf, slot in ((r1_buf, step), (r2_buf, 3 + step)):
                remote(buf.at[0], buf.at[0], px_sem.at[slot], o_sem.at[0], partner).wait_send()

        @pl.loop(0, groups)
        def _(n):
            z_each(n, True)


        @pl.when(far)
        def _():
            w_swap.wait_send()
            for axis in range(2):
                for step in range(3):
                    for copy in w_hop(axis, step):
                        copy.wait_send()

        @pl.when(zh == core)
        def _():
            for copy in w_out:
                copy.wait_send()

        for i in range(g_parts):
            g_swap(i).wait_send()
        for buf, slot in ((kr_buf, 0), (vr_buf, 1)):
            remote(buf, buf, ys_sem.at[slot], o_sem.at[0], partner).wait_send()
            remote(buf, buf, rs_sem.at[slot], o_sem.at[0], partner).wait_send()
        for buf, out, slot in ((dq_buf, dq_ref, 0), (kf_buf, dk_ref, 1), (vf_buf, dv_ref, 2)):
            remote(buf, buf, os_sem.at[slot], o_sem.at[0], partner).wait_send()
            remote(out, out, os_sem.at[slot], o_sem.at[slot], partner).wait_recv()


def copy_kernel(a_ref, b_ref, c_ref, w_ref, a_out, b_out, c_out, w_out, held, in_sem, out_sem):
    moves = []
    for i, (src, dst) in enumerate(((a_ref, a_out), (b_ref, b_out), (c_ref, c_out))):
        for n in range(src.shape[1] // COPY_ROWS):
            rows = pl.ds(n * COPY_ROWS, COPY_ROWS)
            room = held.at[i, rows]
            moves.append(
                (
                    pltpu.make_async_copy(src.at[0, rows], room, in_sem.at[i, n]),
                    pltpu.make_async_copy(room, dst.at[0, rows], out_sem.at[i, n]),
                )
            )
    for move in moves:
        move[0].start()
    w_out[...] = w_ref[...]
    for move in moves:
        move[0].wait()
        move[1].start()
    for move in moves:
        move[1].wait()


def per_device(queries, keys, values, out_grad, proj_weight, lengths):
    tokens, width = queries.shape[1:]
    half = width // 2
    heads = half // HEAD_DIM
    grad_width = out_grad.shape[2]
    groups = heads // 2
    any_space = pl.BlockSpec(memory_space=pl.ANY)
    dma = pltpu.SemaphoreType.DMA
    bf16 = jnp.bfloat16

    def vmem(*shape, dtype=bf16):
        return pltpu.VMEM(shape, dtype)

    pair = vmem(2 * tokens, half)
    outs = jax.ShapeDtypeStruct(queries.shape, bf16)
    weight_grad = jax.ShapeDtypeStruct(
        (grad_width // lax.axis_size("seq"), width // lax.axis_size("dp")), jnp.float32
    )
    results = pl.pallas_call(
        attention_kernel,
        out_shape=(outs, outs, outs, weight_grad),
        in_specs=[any_space] * 5 + [pl.BlockSpec(memory_space=pltpu.SMEM)],
        out_specs=(any_space, any_space, any_space, pl.BlockSpec(memory_space=pltpu.VMEM)),
        scratch_shapes=[
            pair,
            vmem(4 * tokens, half),
            vmem(4 * tokens, half),
            vmem(2 * tokens, grad_width),
            vmem(half, grad_width),
            vmem(half, 2 * tokens),
            vmem(half, 2 * tokens),
            pair,
            pair,
            pair,
            pair,
            pair,
            vmem(2 * tokens, half, dtype=jnp.float32),
            vmem(2 * tokens, half, dtype=jnp.float32),
            pair,
            pair,
            vmem(tokens, grad_width),
            vmem(half, grad_width),
            vmem(3, half, grad_width // 4),
            vmem(3, half, grad_width // 16),
            vmem(2, half // 2, grad_width // 16),
            vmem(4, half // 4, grad_width // 16),
            dma,
            dma((7,)),
            dma((3, groups)),
            dma((3, groups)),
            dma((groups // 2,)),
            dma((6,)),
            dma((heads,)),
            dma((heads,)),
            dma((heads,)),
            dma((4,)),
            dma((4,)),
            dma((3,)),
            dma((7,)),
            dma,
            dma((2,)),
            dma((heads,)),
            dma((heads,)),
            dma((2,)),
            dma((heads,)),
            dma((heads,)),
            dma((3,)),
            dma((3,)),
        ],
        compiler_params=pltpu.CompilerParams(
            collective_id=0, has_side_effects=True, vmem_limit_bytes=66_000_000
        ),
        name="attention",
    )(queries, keys, values, out_grad, proj_weight, lengths)
    pieces = tokens // COPY_ROWS
    dq, dk, dv, turned = pl.pallas_call(
        copy_kernel,
        out_shape=(outs, outs, outs, weight_grad),
        in_specs=[any_space] * 3 + [pl.BlockSpec(memory_space=pltpu.VMEM)],
        out_specs=(any_space, any_space, any_space, pl.BlockSpec(memory_space=pltpu.VMEM)),
        scratch_shapes=[vmem(3, tokens, width), dma((3, pieces)), dma((3, pieces))],
        compiler_params=pltpu.CompilerParams(vmem_limit_bytes=66_000_000),
        cost_estimate=pl.CostEstimate(
            flops=0, bytes_accessed=12 * tokens * width, transcendentals=0
        ),
        name="results",
    )(*results)
    return dq, dk, dv, turned.T


def solution(mesh):
    placed = (
        P("dp", "seq", None),
        P("dp", "seq", None),
        P("dp", "seq", None),
        P("dp", "seq", None),
        P("dp", None),
        P("dp"),
    )
    return jax.shard_map(
        per_device,
        mesh=mesh,
        in_specs=placed,
        out_specs=(
            P("dp", "seq", None),
            P("dp", "seq", None),
            P("dp", "seq", None),
            P("dp", "seq"),
        ),
        check_vma=False,
    )
```

```python
import functools

import jax
import jax.numpy as jnp
from jax import lax
from jax.experimental import pallas as pl
from jax.experimental.pallas import tpu as pltpu
from jax.sharding import PartitionSpec as P

HEAD_DIM = 128
LOG2E = 1.4426950408889634
QUERY_LAG = 2
KEY_LAG = 4
AHEAD = 3
COPY_ROWS = 192
PRODUCTS = (1, 3, 5, 7)
SUMS = (4, 5, 6, 7)
MESH = pl.DeviceIdType.MESH

AB = (((1,), (0,)), ((), ()))
ABT = (((1,), (1,)), ((), ()))


def mm(left, right, dims):
    return lax.dot_general(left, right, dims, preferred_element_type=jnp.float32)


def attention_kernel(
    q_ref,
    k_ref,
    v_ref,
    g_ref,
    w_ref,
    len_ref,
    dq_ref,
    dk_ref,
    dv_ref,
    wg_ref,
    q_buf,
    k_buf,
    v_buf,
    g_buf,
    w_buf,
    do_buf,
    at_buf,
    dq_buf,
    kh_buf,
    vh_buf,
    kr_buf,
    vr_buf,
    ko_buf,
    vo_buf,
    kf_buf,
    vf_buf,
    gm_buf,
    p_buf,
    r1_buf,
    r2_buf,
    zs_buf,
    zr_buf,
    gl_sem,
    px_sem,
    r1_sem,
    r2_sem,
    zr_sem,
    zs_sem,
    kz_sem,
    vz_sem,
    qz_sem,
    g_sem,
    gx_sem,
    w_sem,
    wx_sem,
    wl_sem,
    ys_sem,
    ky_sem,
    vy_sem,
    rs_sem,
    kr_sem,
    vr_sem,
    os_sem,
    o_sem,
):
    seq = lax.axis_index("seq")
    dp = lax.axis_index("dp")
    columns = lax.axis_size("seq") // 2
    zh = lax.rem(seq, 2)
    col = lax.div(seq, 2)
    zl = lax.div(dp, 2)
    core = lax.rem(dp, 2)
    tokens = q_ref.shape[1]
    half = q_ref.shape[2] // 2
    heads = half // HEAD_DIM
    quarter = w_ref.shape[0]
    scale = HEAD_DIM ** (-0.5)

    def device(col_, zh_, zl_, core_):
        return (2 * col_ + zh_, 2 * zl_ + core_)

    targets = [device(col, core, 1 - zl, t) for t in range(2)]
    homes = [device(col, b, 1 - zl, zh) for b in range(2)]
    following = device(lax.rem(col + 1, columns), zh, zl, core)
    previous = device(lax.rem(col + columns - 1, columns), zh, zl, core)
    partner = device(col, zh, zl, 1 - core)

    g_local = pltpu.make_async_copy(g_ref.at[0], gm_buf, gl_sem)
    g_local.start()

    x_at = lax.div(col, 4)
    y_at = lax.rem(col, 4)

    def ring(at, step):
        return lax.rem(at + step + 4, 4)

    x_up, x_down = (device(4 * ring(x_at, i) + y_at, zh, zl, core) for i in (1, -1))
    y_up, y_down = (device(4 * x_at + ring(y_at, i), zh, zl, core) for i in (1, -1))

    barrier = pltpu.get_barrier_semaphore()
    greeted = [following, previous, x_up, x_down, y_up, y_down]
    for i in range(1, 8):
        greeted.append(
            device(
                col,
                1 - zh if i & 4 else zh,
                1 - zl if i & 2 else zl,
                1 - core if i & 1 else core,
            )
        )
    for other in greeted:
        pl.semaphore_signal(barrier, inc=1, device_id=other, device_id_type=MESH)
    with jax.named_scope("barrier"):
        pl.semaphore_wait(barrier, len(greeted))

    def remote(src, dst, send_sem, recv_sem, to):
        return pltpu.make_async_remote_copy(
            src_ref=src,
            dst_ref=dst,
            send_sem=send_sem,
            recv_sem=recv_sem,
            device_id=to,
            device_id_type=MESH,
        )

    def lanes(h):
        return pl.ds(pl.multiple_of(h * HEAD_DIM, HEAD_DIM), HEAD_DIM)

    my_rows = pl.ds(pl.multiple_of(zh * tokens, tokens), tokens)
    own_rows = pl.ds(2 * tokens, 2 * tokens)
    halo_rows = pl.ds(0, 2 * tokens)
    my_half = pl.ds(pl.multiple_of(core * half, half), half)

    def send_home(ref, buf, base, h, recv_sem, slot):
        rows = pl.ds(pl.multiple_of(base + zh * tokens, tokens), tokens)
        for t in range(2):
            src = pl.ds(pl.multiple_of(t * half + h * HEAD_DIM, HEAD_DIM), HEAD_DIM)
            remote(
                ref.at[0, :, src],
                buf.at[rows, lanes(h)],
                zs_sem.at[slot],
                recv_sem.at[h],
                targets[t],
            ).start()

    far = core != zl
    piece_rows = quarter // 8
    w_rows = pl.ds(pl.multiple_of(core * quarter, quarter), quarter)
    w_local = pltpu.make_async_copy(w_ref, w_buf.at[w_rows], wl_sem)
    w_swap = remote(w_ref, w_buf.at[w_rows], zs_sem.at[4], w_sem.at[2], partner)
    w_axes = ((x_at, x_down), (y_at, y_down))

    def w_piece(axis, j, at):
        first_row = j * quarter + axis * (quarter // 2) + at * piece_rows
        return w_buf.at[pl.ds(pl.multiple_of(first_row, piece_rows), piece_rows)]

    def w_source(axis):
        first_row = axis * (quarter // 2) + w_axes[axis][0] * piece_rows
        return w_ref.at[pl.ds(pl.multiple_of(first_row, piece_rows), piece_rows)]

    w_out = [
        remote(
            w_source(axis),
            w_piece(axis, core, w_axes[axis][0]),
            zs_sem.at[4],
            w_sem.at[axis],
            device(col, b, 1 - zl, zl),
        )
        for axis in range(2)
        for b in range(2)
    ]

    def w_hop(axis, step):
        at, down = w_axes[axis]
        pieces = [w_piece(axis, j, ring(at, step)) for j in range(2)]
        return [
            remote(piece, piece, wx_sem.at[6], wx_sem.at[2 * step + axis], down)
            for piece in pieces
        ]

    def w_wait(sem):
        pieces = w_buf.at[pl.ds(0, 2 * piece_rows)]
        with jax.named_scope("w_wait"):
            remote(pieces, pieces, zs_sem.at[4], sem, partner).wait_recv()

    def w_step(step):
        @pl.when(far)
        def _():
            for axis in range(2):
                w_wait(w_sem.at[axis] if step == 0 else wx_sem.at[2 * step - 2 + axis])
                if step < 3:
                    for copy in w_hop(axis, step):
                        copy.start()

    @pl.when(far)
    def _():
        w_swap.start()

    @pl.when(jnp.logical_not(far))
    def _():
        w_local.start()

    @pl.when(zh == core)
    def _():
        for copy in w_out:
            copy.start()

    def send_keys(h):
        send_home(k_ref, k_buf, 2 * tokens, h, kz_sem, 0)
        send_home(v_ref, v_buf, 2 * tokens, h, vz_sem, 1)

    def send_queries(h):
        send_home(q_ref, q_buf, 0, h, qz_sem, 2)

    g_parts = 4
    g_width = half // g_parts
    send_keys(0)
    g_local.wait()
    limit = len_ref[0] - seq * tokens
    live = lax.broadcasted_iota(jnp.int32, gm_buf.shape, 0) < limit
    gm_buf[...] = jnp.where(live, gm_buf[...], jnp.zeros_like(gm_buf))
    for i in range(g_parts):
        for t in range(2):
            cols = pl.ds(t * half + i * g_width, g_width)
            remote(
                gm_buf.at[:, cols], g_buf.at[my_rows, cols], zs_sem.at[3], g_sem.at[i], targets[t]
            ).start()
        if i + 1 < g_parts:
            send_keys(i + 1)
    send_queries(0)

    @pl.loop(g_parts, heads)
    def _(h):
        send_keys(h)
        for i in range(2):
            n = 2 * (h - g_parts) + 1 + i

            @pl.when(n < heads)
            def _():
                send_queries(n)

    def forward(h):
        for buf, got, sem, slot in (
            (k_buf, kz_sem, ky_sem, 0),
            (v_buf, vz_sem, vy_sem, 1),
        ):
            own = buf.at[own_rows, lanes(h)]
            with jax.named_scope("kv_wait"):
                remote(own, own, zs_sem.at[0], got.at[h], partner).wait_recv()
            remote(own, buf.at[halo_rows, lanes(h)], ys_sem.at[slot], sem.at[h], following).start()

    def g_piece(i):
        cols = pl.ds(pl.multiple_of(core * half + i * g_width, g_width), g_width)
        return g_buf.at[:, cols]

    def g_swap(i):
        return remote(g_piece(i), g_piece(i), zs_sem.at[5], gx_sem.at[i], partner)

    def g_exchange(i):
        with jax.named_scope("g_wait"):
            remote(g_piece(i), g_piece(i), zs_sem.at[3], g_sem.at[i], partner).wait_recv()
        g_swap(i).start()

    w_step(0)
    forward(0)
    w_step(1)
    g_exchange(0)
    forward(1)
    w_step(2)
    g_exchange(1)
    w_step(3)
    forward(2)
    g_exchange(2)
    forward(3)
    g_exchange(3)

    @pl.when(jnp.logical_not(far))
    def _():
        w_local.wait()
        remote(w_ref, w_ref, zs_sem.at[4], w_sem.at[2], partner).wait_recv()

    with jax.named_scope("gx_wait"):
        for i in range(g_parts):
            g_swap(i).wait_recv()

    with jax.named_scope("out_bwd"):

        @pl.loop(0, 2 * tokens // 256)
        def _(n):
            rows = pl.ds(pl.multiple_of(n * 256, 256), 256)
            do_buf[:, rows] = mm(w_buf[...], g_buf[rows, :], ABT).astype(jnp.bfloat16)

    first = jnp.where(col == 0, -1e30, 0.0).astype(jnp.float32)
    key_pos = lax.broadcasted_iota(jnp.int32, (tokens, tokens), 0)
    query_pos = lax.broadcasted_iota(jnp.int32, (tokens, tokens), 1)

    def head(h):
        at = lanes(h)
        feats = pl.ds(pl.multiple_of(h * HEAD_DIM, HEAD_DIM), HEAD_DIM)
        value_t = v_buf[:, at].T
        key_t = k_buf[:, at].T
        dk = [None] * 4
        dv = [None] * 4

        def add(total, block, term):
            total[block] = term if total[block] is None else total[block] + term

        for b in range(2):
            rows = slice(b * tokens, (b + 1) * tokens)
            q = q_buf[rows, at]
            do = do_buf[feats, rows]
            blocks = [b, b + 1, b + 2]
            tile = [slice(n * tokens, (n + 1) * tokens) for n in blocks]
            scores = []
            for j in range(3):
                s = mm(k_buf[tile[j], at], q, ABT)
                if blocks[j] < 2:
                    s = s + first
                if j == 2:
                    s = jnp.where(key_pos <= query_pos, s, -1e30)
                scores.append(s)
            top = scores[0].max(axis=0, keepdims=True)
            for s in scores[1:]:
                top = jnp.maximum(top, s.max(axis=0, keepdims=True))
            probs = [jnp.exp2((s - top) * (scale * LOG2E)) for s in scores]
            total = probs[0].sum(axis=0, keepdims=True)
            for p in probs[1:]:
                total = total + p.sum(axis=0, keepdims=True)
            inverse = 1.0 / total
            probs = [p * inverse for p in probs]
            attn = None
            for j in range(3):
                probs_b = probs[j].astype(jnp.bfloat16)
                term = mm(value_t[:, tile[j]], probs_b, AB)
                attn = term if attn is None else attn + term
                add(dv, blocks[j], mm(probs_b, do, ABT))
            attn = attn.astype(jnp.bfloat16)
            at_buf[feats, rows] = attn
            delta = jnp.sum(
                do.astype(jnp.float32) * attn.astype(jnp.float32), axis=0, keepdims=True
            )
            dq = None
            for j in range(3):
                grad = mm(v_buf[tile[j], at], do, AB)
                sg = (probs[j] * (grad - delta)).astype(jnp.bfloat16)
                term = mm(key_t[:, tile[j]], sg, AB)
                dq = term if dq is None else dq + term
                add(dk, blocks[j], mm(sg, q, AB))
            dq_buf[rows, at] = (dq * scale).T.astype(jnp.bfloat16)
        for n in range(2):
            rows = slice(n * tokens, (n + 1) * tokens)
            kh_buf[rows, at] = (dk[n] * scale).astype(jnp.bfloat16)
            vh_buf[rows, at] = dv[n].astype(jnp.bfloat16)
            ko_buf[rows, at] = dk[n + 2] * scale
            vo_buf[rows, at] = dv[n + 2]

    def send_out(buf, out, slot, h):
        cols = pl.ds(pl.multiple_of(core * half + h * HEAD_DIM, HEAD_DIM), HEAD_DIM)
        for b in range(2):
            remote(
                buf.at[pl.ds(b * tokens, tokens), lanes(h)],
                out.at[0, :, cols],
                os_sem.at[slot],
                o_sem.at[slot],
                homes[b],
            ).start()

    def finish(h):
        at = lanes(h)
        for got, own, done, out, sem, slot in (
            (kr_buf, ko_buf, kf_buf, dk_ref, kr_sem, 1),
            (vr_buf, vo_buf, vf_buf, dv_ref, vr_sem, 2),
        ):
            piece = got.at[:, at]
            with jax.named_scope("back_wait"):
                remote(piece, piece, rs_sem.at[0], sem.at[h], partner).wait_recv()
            done[:, at] = (own[:, at] + got[:, at].astype(jnp.float32)).astype(jnp.bfloat16)
            send_out(done, out, slot, h)

    def give_back(t):
        for lag, task in ((QUERY_LAG, lambda h: send_out(dq_buf, dq_ref, 0, h)), (KEY_LAG, finish)):

            @pl.when((t >= lag) & (t - lag < heads))
            def _():
                task(t - lag)

    group = 2 * HEAD_DIM
    groups = half // group
    wide = 128
    part = 4 * wide
    along_x = core == 0
    outer_at = jnp.where(along_x, x_at, y_at)
    inner_at = jnp.where(along_x, y_at, x_at)

    def device_of(first, second):
        return tuple(jnp.where(along_x, a, b) for a, b in zip(first, second))

    outer_up = device_of(x_up, y_up)
    inner_up = device_of(y_up, x_up)

    def group_rows(n):
        return pl.ds(pl.multiple_of(n * group, group), group)

    def columns_of(n, size):
        return pl.ds(pl.multiple_of(n * size, size), size)

    def f32(value):
        return value.astype(jnp.float32)

    def landed(ref, sem):
        with jax.named_scope("sum_wait"):
            remote(ref, ref, px_sem.at[0], sem, partner).wait_recv()

    def outer_send(n, step, src):
        remote(
            src, r1_buf.at[step, group_rows(n)], px_sem.at[step], r1_sem.at[step, n], outer_up
        ).start()

    def inner_send(n, step, src):
        remote(
            src, r2_buf.at[step, group_rows(n)], px_sem.at[3 + step], r2_sem.at[step, n], inner_up
        ).start()

    def product(n):
        rows = group_rows(n)

        @pl.loop(0, 4)
        def _(x):
            term = mm(at_buf[rows, :], g_buf[:, columns_of(x, part)], AB).astype(jnp.bfloat16)
            for y in range(4):
                place = jnp.where(along_x, 4 * x + y, 4 * y + x)
                p_buf[rows, columns_of(place, wide)] = term[:, y * wide : (y + 1) * wide]

        outer_send(n, 0, p_buf.at[rows, columns_of(ring(outer_at, -1), part)])

    def outer(step, n):
        rows = group_rows(n)
        landed(r1_buf.at[step, rows], r1_sem.at[step, n])
        cols = columns_of(ring(outer_at, -2 - step), part)
        total = f32(p_buf[rows, cols]) + f32(r1_buf[step, rows, :])
        r1_buf[step, rows, :] = total.astype(jnp.bfloat16)
        if step < 2:
            outer_send(n, step + 1, r1_buf.at[step, rows])
        else:
            inner_send(n, 0, r1_buf.at[2, rows, columns_of(ring(inner_at, -1), wide)])

    def inner(step, n):
        rows = group_rows(n)
        landed(r2_buf.at[step, rows], r2_sem.at[step, n])
        cols = columns_of(ring(inner_at, -2 - step), wide)
        total = f32(r1_buf[2, rows, cols]) + f32(r2_buf[step, rows, :])
        if step < 2:
            r2_buf[step, rows, :] = total.astype(jnp.bfloat16)
            inner_send(n, step + 1, r2_buf.at[step, rows])
        else:
            z_send(n, total)

    short = group // 2

    def packed_rows(n):
        return pl.ds(pl.multiple_of(n * short, short), short)

    def z_each(n, sent):
        owner = lax.div(n, groups // 2)
        slot_rows = packed_rows(lax.rem(n, groups // 2))
        for b in range(2):
            own = (zl == core) & (owner == core) & (zh == b)
            copy = remote(
                zs_buf.at[b, packed_rows(n)],
                zr_buf.at[2 * zh + zl, slot_rows],
                px_sem.at[6],
                zr_sem.at[lax.rem(n, groups // 2)],
                device(col, b, core, owner),
            )

            @pl.when(jnp.logical_not(own))
            def _():
                if sent:
                    copy.wait_send()
                else:
                    copy.start()

            if not sent:

                @pl.when(own)
                def _():
                    zr_buf[2 * zh + zl, slot_rows, :] = zs_buf[b, packed_rows(n), :]

    def z_send(n, total):
        upper, lower = total[:short], total[short:]
        left = lax.broadcasted_iota(jnp.int32, upper.shape, 1) < wide // 2
        for b, packed in enumerate(
            (
                jnp.where(left, upper, pltpu.roll(lower, wide // 2, 1)),
                jnp.where(left, pltpu.roll(upper, wide // 2, 1), lower),
            )
        ):
            zs_buf[b, packed_rows(n), :] = packed.astype(jnp.bfloat16)
        z_each(n, False)

    stages = [product]
    stages += [lambda n, step=step: outer(step, n) for step in range(3)]
    stages += [lambda n, step=step: inner(step, n) for step in range(3)]

    def reduce_step(t):
        for late, stage in enumerate(stages):
            times = SUMS if late else PRODUCTS
            due = functools.reduce(jnp.logical_or, [t - late == time for time in times])
            n = sum((t - late > time).astype(jnp.int32) for time in times)

            @pl.when(due)
            def _():
                with jax.named_scope(f"stage{late}"):
                    stage(n)

    @pl.loop(0, heads)
    def _(h):
        @pl.when((h >= 1) & (h + AHEAD < heads))
        def _():
            forward(h + AHEAD)

        at = lanes(h)
        piece = q_buf.at[:, at]
        with jax.named_scope("q_wait"):
            remote(piece, piece, zs_sem.at[2], qz_sem.at[h], partner).wait_recv()
        for buf, sem in ((k_buf, ky_sem), (v_buf, vy_sem)):
            piece = buf.at[halo_rows, at]
            with jax.named_scope("halo_wait"):
                remote(piece, piece, ys_sem.at[0], sem.at[h], partner).wait_recv()
        with jax.named_scope("head"):
            head(h)
        for src, dst, sem, slot in ((kh_buf, kr_buf, kr_sem, 0), (vh_buf, vr_buf, vr_sem, 1)):
            remote(
                src.at[:, at], dst.at[:, at], rs_sem.at[slot], sem.at[h], previous
            ).start()
        give_back(h)

        reduce_step(h)

    @pl.loop(heads, heads + max(KEY_LAG, SUMS[-1] + len(stages) - heads))
    def _(t):
        give_back(t)
        reduce_step(t)

    for n in range(groups // 2):
        rows = pl.ds(n * short, short)
        every = zr_buf.at[:, rows]
        some = zr_buf.at[pl.ds(0, 3), rows]

        @pl.when(zl == core)
        def _():
            landed(some, zr_sem.at[n])

        @pl.when(zl != core)
        def _():
            landed(every, zr_sem.at[n])

        total = f32(zr_buf[0, rows, :])
        for i in range(1, 4):
            total = total + f32(zr_buf[i, rows, :])
        turned = total.T
        wg_ref[:, pl.ds(n * group, short)] = turned[: wide // 2]
        wg_ref[:, pl.ds(n * group + short, short)] = turned[wide // 2 :]

    with jax.named_scope("drain"):
        for ref, slot in ((k_ref, 0), (v_ref, 1), (q_ref, 2)):
            remote(ref, ref, zs_sem.at[slot], o_sem.at[0], partner).wait_send()
        remote(gm_buf, gm_buf, zs_sem.at[3], o_sem.at[0], partner).wait_send()
        for step in range(3):
            for buf, slot in ((r1_buf, step), (r2_buf, 3 + step)):
                remote(buf.at[0], buf.at[0], px_sem.at[slot], o_sem.at[0], partner).wait_send()

        @pl.loop(0, groups)
        def _(n):
            z_each(n, True)


        @pl.when(far)
        def _():
            w_swap.wait_send()
            for axis in range(2):
                for step in range(3):
                    for copy in w_hop(axis, step):
                        copy.wait_send()

        @pl.when(zh == core)
        def _():
            for copy in w_out:
                copy.wait_send()

        for i in range(g_parts):
            g_swap(i).wait_send()
        for buf, slot in ((kr_buf, 0), (vr_buf, 1)):
            remote(buf, buf, ys_sem.at[slot], o_sem.at[0], partner).wait_send()
            remote(buf, buf, rs_sem.at[slot], o_sem.at[0], partner).wait_send()
        for buf, out, slot in ((dq_buf, dq_ref, 0), (kf_buf, dk_ref, 1), (vf_buf, dv_ref, 2)):
            remote(buf, buf, os_sem.at[slot], o_sem.at[0], partner).wait_send()
            remote(out, out, os_sem.at[slot], o_sem.at[slot], partner).wait_recv()


def copy_kernel(a_ref, b_ref, c_ref, w_ref, a_out, b_out, c_out, w_out, held, in_sem, out_sem):
    moves = []
    for i, (src, dst) in enumerate(((a_ref, a_out), (b_ref, b_out), (c_ref, c_out))):
        for n in range(src.shape[1] // COPY_ROWS):
            rows = pl.ds(n * COPY_ROWS, COPY_ROWS)
            room = held.at[i, rows]
            moves.append(
                (
                    pltpu.make_async_copy(src.at[0, rows], room, in_sem.at[i, n]),
                    pltpu.make_async_copy(room, dst.at[0, rows], out_sem.at[i, n]),
                )
            )
    for move in moves:
        move[0].start()
    w_out[...] = w_ref[...]
    for move in moves:
        move[0].wait()
        move[1].start()
    for move in moves:
        move[1].wait()


def per_device(queries, keys, values, out_grad, proj_weight, lengths):
    tokens, width = queries.shape[1:]
    half = width // 2
    heads = half // HEAD_DIM
    grad_width = out_grad.shape[2]
    groups = heads // 2
    any_space = pl.BlockSpec(memory_space=pl.ANY)
    dma = pltpu.SemaphoreType.DMA
    bf16 = jnp.bfloat16

    def vmem(*shape, dtype=bf16):
        return pltpu.VMEM(shape, dtype)

    pair = vmem(2 * tokens, half)
    outs = jax.ShapeDtypeStruct(queries.shape, bf16)
    weight_grad = jax.ShapeDtypeStruct(
        (grad_width // lax.axis_size("seq"), width // lax.axis_size("dp")), jnp.float32
    )
    results = pl.pallas_call(
        attention_kernel,
        out_shape=(outs, outs, outs, weight_grad),
        in_specs=[any_space] * 5 + [pl.BlockSpec(memory_space=pltpu.SMEM)],
        out_specs=(any_space, any_space, any_space, pl.BlockSpec(memory_space=pltpu.VMEM)),
        scratch_shapes=[
            pair,
            vmem(4 * tokens, half),
            vmem(4 * tokens, half),
            vmem(2 * tokens, grad_width),
            vmem(half, grad_width),
            vmem(half, 2 * tokens),
            vmem(half, 2 * tokens),
            pair,
            pair,
            pair,
            pair,
            pair,
            vmem(2 * tokens, half, dtype=jnp.float32),
            vmem(2 * tokens, half, dtype=jnp.float32),
            pair,
            pair,
            vmem(tokens, grad_width),
            vmem(half, grad_width),
            vmem(3, half, grad_width // 4),
            vmem(3, half, grad_width // 16),
            vmem(2, half // 2, grad_width // 16),
            vmem(4, half // 4, grad_width // 16),
            dma,
            dma((7,)),
            dma((3, groups)),
            dma((3, groups)),
            dma((groups // 2,)),
            dma((6,)),
            dma((heads,)),
            dma((heads,)),
            dma((heads,)),
            dma((4,)),
            dma((4,)),
            dma((3,)),
            dma((7,)),
            dma,
            dma((2,)),
            dma((heads,)),
            dma((heads,)),
            dma((2,)),
            dma((heads,)),
            dma((heads,)),
            dma((3,)),
            dma((3,)),
        ],
        compiler_params=pltpu.CompilerParams(
            collective_id=0, has_side_effects=True, vmem_limit_bytes=66_000_000
        ),
        name="attention",
    )(queries, keys, values, out_grad, proj_weight, lengths)
    pieces = tokens // COPY_ROWS
    dq, dk, dv, turned = pl.pallas_call(
        copy_kernel,
        out_shape=(outs, outs, outs, weight_grad),
        in_specs=[any_space] * 3 + [pl.BlockSpec(memory_space=pltpu.VMEM)],
        out_specs=(any_space, any_space, any_space, pl.BlockSpec(memory_space=pltpu.VMEM)),
        scratch_shapes=[vmem(3, tokens, width), dma((3, pieces)), dma((3, pieces))],
        compiler_params=pltpu.CompilerParams(vmem_limit_bytes=66_000_000),
        cost_estimate=pl.CostEstimate(
            flops=0, bytes_accessed=12 * tokens * width, transcendentals=0
        ),
        name="results",
    )(*results)
    return dq, dk, dv, turned.T


def solution(mesh):
    placed = (
        P("dp", "seq", None),
        P("dp", "seq", None),
        P("dp", "seq", None),
        P("dp", "seq", None),
        P("dp", None),
        P("dp"),
    )
    return jax.shard_map(
        per_device,
        mesh=mesh,
        in_specs=placed,
        out_specs=(
            P("dp", "seq", None),
            P("dp", "seq", None),
            P("dp", "seq", None),
            P("dp", "seq"),
        ),
        check_vma=False,
    )
```
